32 devices in a mesh: height: 4 (over x, core), dom: 8 (over z, y).
Axes of the slice: x: 2, y: 2, z: 4, core: 2. Of those that a mesh axis runs over, the one named last changes fastest.
Arguments:
- modes_now: float32 [64, 64, 4096], P('height', 'dom'), may hold values from -6 to 6
- modes_prev: float32 [64, 64, 4096], P('height', 'dom'), may hold values from -6 to 6
- partition_boxes: int32 [64, 2], P('dom'), may hold values from 16 to 64, as said below
- face_table: int32 [256, 8], P('dom'), may hold values from 0 to 64, as said below
Outputs:
- new_modes: float32 [64, 64, 4096], P('height', 'dom')
- pressure: float32 [64, 64, 4096], P('height', 'dom')
The draws below stay inside these ranges and needn't reach their ends.
Inputs may be any that keep to these rules, and one draw needn't show every extreme that they name: `partition_boxes`: column 0 is a partition's extent along x, column 1 along y. `face_table`: row r belongs to dom index r // 32. Columns: 0 the local number of the source partition on that index, 1 its side (0 low x, 1 high x, 2 low y, 3 high y), 2 the first cell of the face along that side, 3 the face's length in cells (0 marks an unused row), 4 the dom index holding the target partition, 5 the target's local number, 6 its side, 7 the first cell along it. Sides 0 and 1 run along y, sides 2 and 3 along x; start plus length never passes either side's extent. Among the rows of one dom index at most 4 name the same dom index in column 4, and that many is reached in every draw.
All inputs are finite; a program needn't handle non-finite values.
Results may differ from the reference program's by a relative error of at most 0.0002.
Values sent between devices are 32-bit elements; how exact they have to be, the bound alone decides.
A program may use at most 64 MiB of HBM per device.

```python
import jax
import jax.numpy as jnp
from jax import lax

B = 64
NZ = 64
PDEV = 8
FDEV = 32
PARTS_SIZE = 64
N_DOM = 8


def layout_tables(key):
    extents = jax.random.randint(jax.random.fold_in(key, 101), (N_DOM * PDEV, 2), B // 4, B + 1)
    pair_most = max(2, FDEV // N_DOM)
    groups = FDEV // pair_most
    order_key = jax.random.fold_in(key, 202)
    sources = jnp.arange(N_DOM, dtype=jnp.int32)

    def shuffled(source):
        return jax.random.permutation(jax.random.fold_in(order_key, source), N_DOM).astype(jnp.int32)
    offsets = jax.vmap(shuffled)(sources)[:, :groups]
    slot_ids = jnp.arange(FDEV, dtype=jnp.int32)
    group_of = slot_ids // pair_most
    targets = (sources[:, None] + offsets[:, group_of]) % N_DOM
    live_count = jax.random.randint(jax.random.fold_in(key, 303), (N_DOM, groups), 1, pair_most + 1)
    live_count = live_count.at[:, 0].set(pair_most)
    alive = (slot_ids % pair_most)[None, :] < live_count[:, group_of]
    grid_shape = (N_DOM, FDEV)
    src_part = jax.random.randint(jax.random.fold_in(key, 404), grid_shape, 0, PDEV)
    src_side = jax.random.randint(jax.random.fold_in(key, 505), grid_shape, 0, 4)
    dst_part = jax.random.randint(jax.random.fold_in(key, 606), grid_shape, 0, PDEV)
    dst_side = jax.random.randint(jax.random.fold_in(key, 707), grid_shape, 0, 4)
    src_global = sources[:, None] * PDEV + src_part
    dst_global = targets * PDEV + dst_part
    src_extent = jnp.where(src_side < 2, extents[src_global, 1], extents[src_global, 0])
    dst_extent = jnp.where(dst_side < 2, extents[dst_global, 1], extents[dst_global, 0])
    seg_length = jax.random.randint(jax.random.fold_in(key, 808), grid_shape, 1, jnp.minimum(src_extent, dst_extent) + 1)
    seg_length = jnp.where(alive, seg_length, 0)
    src_start = jax.random.randint(jax.random.fold_in(key, 909), grid_shape, 0, src_extent - seg_length + 1)
    dst_start = jax.random.randint(jax.random.fold_in(key, 1001), grid_shape, 0, dst_extent - seg_length + 1)
    face_rows = jnp.stack([src_part, src_side, src_start, seg_length, targets, dst_part, dst_side, dst_start], -1)
    return (extents.astype(jnp.int32), face_rows.reshape(N_DOM * FDEV, 8).astype(jnp.int32))


def draw_partition_boxes(key, part):
    return layout_tables(key)[0]


def draw_face_table(key, part):
    return layout_tables(key)[1]


def block_levels(stream_key, extent, pieces, smallest, largest):
    def one(dim, parts):
        steps = jax.random.uniform(jax.random.fold_in(jax.random.fold_in(stream_key, 6), dim), (parts,), jnp.float32, smallest / len(pieces), largest / len(pieces))
        return jnp.repeat(jnp.exp(steps), extent[dim] // parts).reshape((-1,) + (1,) * (len(extent) - dim - 1))

    gain = one(*pieces[0])
    for cut in pieces[1:]:
        gain = gain * one(*cut)
    return gain


def centred(own_key, dims, spread, most, pieces=(), held_as=jnp.bfloat16):
    entries = jax.random.normal(own_key, dims, jnp.float32) * spread
    if len(pieces) > 0:
        entries = block_levels(own_key, dims, pieces, -0.22, 0.18) * entries
    return jnp.clip(entries, min=-most, max=most).astype(held_as)


def setup_inputs(seed: int = 0) -> dict:
    arg_keys = jax.random.split(jax.random.key(seed), 5)
    return {
        "modes_now": centred(arg_keys[0], (NZ, PARTS_SIZE, B * B), 1.0, 6.0, ((0, 4), (1, 8)), jnp.float32),
        "modes_prev": centred(arg_keys[1], (NZ, PARTS_SIZE, B * B), 1.0, 6.0, ((0, 4), (1, 8)), jnp.float32),
        "partition_boxes": draw_partition_boxes(jax.random.fold_in(arg_keys[4], 71), 0),
        "face_table": draw_face_table(jax.random.fold_in(arg_keys[4], 71), 0),
    }


COUPLING = 32.0
STENCIL = (COUPLING * 270.0 / 180.0, COUPLING * -27.0 / 180.0, COUPLING * 2.0 / 180.0)
TIME_STEP = 0.4

def cosine_table(lengths, box_side):
    lengths = lengths.astype(jnp.float32)[..., None, None]
    ordinal = jnp.arange(box_side, dtype=jnp.float32)
    waves = ordinal[:, None]
    places = ordinal[None, :]
    scales = jnp.sqrt(jnp.where(waves == 0, 1.0, 2.0) / lengths)
    values = scales * jnp.cos(jnp.pi * waves * (places + 0.5) / lengths)
    inside = (waves < lengths) & (places < lengths)
    return jnp.where(inside, values, 0.0)

def mix_planes(matrix, grid_field):
    flat = grid_field.reshape(matrix.shape[1], -1)
    mixed = jnp.dot(matrix, flat, precision=lax.Precision.HIGHEST, preferred_element_type=jnp.float32)
    return mixed.reshape(matrix.shape[0], grid_field.shape[1], grid_field.shape[2])

def to_cells(table_rows, table_cols, grid_field, box_side):
    planes, holders, cells = grid_field.shape
    squares = grid_field.reshape(planes, holders, box_side, box_side)
    halfway = jnp.einsum('pka,zpkl->zpal', table_rows, squares, precision=lax.Precision.HIGHEST)
    complete = jnp.einsum('zpal,plb->zpab', halfway, table_cols, precision=lax.Precision.HIGHEST)
    return complete.reshape(planes, holders, cells)

def to_modes(table_rows, table_cols, grid_field, box_side):
    planes, holders, cells = grid_field.shape
    squares = grid_field.reshape(planes, holders, box_side, box_side)
    halfway = jnp.einsum('pka,zpab->zpkb', table_rows, squares, precision=lax.Precision.HIGHEST)
    complete = jnp.einsum('zpkb,plb->zpkl', halfway, table_cols, precision=lax.Precision.HIGHEST)
    return complete.reshape(planes, holders, cells)

def side_cells(facing, offsets, amounts, extent_rows, extent_cols, box_side):
    number = facing.shape[0]
    layers = jnp.arange(3, dtype=jnp.int32)[None, :, None]
    position = jnp.arange(box_side, dtype=jnp.int32)[None, None, :]
    facing = facing[:, None, None]
    reached = offsets[:, None, None] + position
    coord_rows = jnp.where(facing == 0, layers, jnp.where(facing == 1, extent_rows[:, None, None] - 1 - layers, reached))
    coord_cols = jnp.where(facing == 2, layers, jnp.where(facing == 3, extent_cols[:, None, None] - 1 - layers, reached))
    usable = jnp.broadcast_to((position < amounts[:, None, None]) & (layers >= 0), (number, 3, box_side))
    cell_index = jnp.where(usable, coord_rows * box_side + coord_cols, 0)
    return (cell_index.reshape(number, 3 * box_side).astype(jnp.int32), usable.reshape(number, 3 * box_side))

def face_forcing(pressure, aligned, targets, facing, offsets, amounts, extent_rows, extent_cols, box_side):
    planes = pressure.shape[0]
    number = targets.shape[0]
    cell_index, usable = side_cells(facing, offsets, amounts, extent_rows[targets], extent_cols[targets], box_side)
    inside_rim = jnp.where(usable, pressure[:, targets[:, None], cell_index], 0.0)
    jumps = (aligned - inside_rim).reshape(planes, number, 3, box_side)
    nearest = jumps[:, :, 0]
    second = jumps[:, :, 1]
    farthest = jumps[:, :, 2]
    closest = STENCIL[0] * nearest + STENCIL[1] * second + STENCIL[2] * farthest
    middle = STENCIL[1] * nearest + STENCIL[2] * second
    outer = STENCIL[2] * nearest
    pushes = jnp.stack([closest, middle, outer], 2).reshape(planes, number, 3 * box_side)
    pushes = jnp.where(usable, pushes, 0.0)
    return jnp.zeros_like(pressure).at[:, targets[:, None], cell_index].add(pushes)

def advance(modes_now, modes_prev, force_modes, extent_rows, extent_cols, first_plane, total_planes, box_side):
    planes, holders, cells = modes_now.shape
    wave_depth = (first_plane + jnp.arange(planes, dtype=jnp.int32)).astype(jnp.float32) / total_planes
    wave_side = jnp.arange(box_side, dtype=jnp.float32)
    float_rows = extent_rows.astype(jnp.float32)
    float_cols = extent_cols.astype(jnp.float32)
    ratio_rows = wave_side[None, :] / float_rows[:, None]
    ratio_cols = wave_side[None, :] / float_cols[:, None]
    squared = jnp.pi ** 2 * (wave_depth[:, None, None, None] ** 2 + ratio_rows[None, :, :, None] ** 2 + ratio_cols[None, :, None, :] ** 2)
    phases = jnp.sqrt(squared) * TIME_STEP
    growth = TIME_STEP * TIME_STEP * jnp.sinc(phases / (2.0 * jnp.pi)) ** 2
    inside = (wave_side[None, :, None] < float_rows[:, None, None]) & (wave_side[None, None, :] < float_cols[:, None, None])
    grid_shape = (planes, holders, box_side, box_side)
    updated = 2.0 * jnp.cos(phases) * modes_now.reshape(grid_shape) - modes_prev.reshape(grid_shape) + growth * force_modes.reshape(grid_shape)
    return jnp.where(inside[None], updated, 0.0).reshape(planes, holders, cells)

def reference(modes_now, modes_prev, partition_boxes, face_table):
    extent_rows = partition_boxes[:, 0]
    extent_cols = partition_boxes[:, 1]
    table_rows = cosine_table(extent_rows, B)
    table_cols = cosine_table(extent_cols, B)
    table_depth = cosine_table(jnp.full((), NZ, jnp.int32), NZ)
    plane_modes = mix_planes(table_depth.T, modes_now)
    pressure = to_cells(table_rows, table_cols, plane_modes, B)
    row_ids = jnp.arange(N_DOM * FDEV, dtype=jnp.int32)
    holder = row_ids // FDEV
    sources = holder * PDEV + face_table[:, 0]
    src_index, src_usable = side_cells(face_table[:, 1], face_table[:, 2], face_table[:, 3], extent_rows[sources], extent_cols[sources], B)
    aligned = jnp.where(src_usable, pressure[:, sources[:, None], src_index], 0.0)
    targets = face_table[:, 4] * PDEV + face_table[:, 5]
    forcing = face_forcing(pressure, aligned, targets, face_table[:, 6], face_table[:, 7], face_table[:, 3], extent_rows, extent_cols, B)
    force_modes = mix_planes(table_depth, to_modes(table_rows, table_cols, forcing, B))
    new_modes = advance(modes_now, modes_prev, force_modes, extent_rows, extent_cols, jnp.zeros((), jnp.int32), NZ, B)
    return (new_modes, pressure)
```

```python
import functools
import math

import jax
import jax.numpy as jnp
from jax import lax
from jax.experimental import pallas as pl
from jax.experimental.pallas import tpu as pltpu
from jax.sharding import PartitionSpec as P

COUPLING = 32.0
STENCIL = (COUPLING * 270.0 / 180.0, COUPLING * -27.0 / 180.0, COUPLING * 2.0 / 180.0)
TIME_STEP = 0.4
SERIES = (1.0, -1.0 / 6, 1.0 / 120, -1.0 / 5040, 1.0 / 362880, -1.0 / 39916800, 1.0 / 6227020800)
GROUP = 4
SIDES = 12


def iota(shape, axis):
    return lax.broadcasted_iota(jnp.int32, shape, axis)


def whole(shape):
    return pl.BlockSpec(shape, lambda *_: (0,) * len(shape))


def split(values):
    high = values.astype(jnp.bfloat16)
    return high, (values - high.astype(jnp.float32)).astype(jnp.bfloat16)


def halves(values):
    return jnp.concatenate(split(values), 0)


def dot(left, right):
    return jnp.dot(left, right, preferred_element_type=jnp.float32)


def thrice(values):
    high, low = split(values)
    return jnp.concatenate([high, low, high], 1)


def stacked(pair):
    size = pair.shape[0] // 2
    return jnp.concatenate([pair[:size], pair[:size], pair[size:]], 0)


def cosines(wave, place, length):
    span = jnp.full((1, wave.shape[1]), length, jnp.int32).astype(jnp.float32)
    inverse = 0.25 / span
    wave = wave.astype(jnp.float32)
    place = place.astype(jnp.float32)
    turns = wave * (2.0 * place + 1.0)
    rest = (turns - jnp.floor(turns * inverse + 0.5) * (4.0 * span)) * (inverse * math.pi)
    square = rest * rest
    sine = jnp.float32(1.0 / math.factorial(13))
    for order in (11, 9, 7, 5, 3, 1):
        sine = sine * square + (-1.0) ** (order // 2) / math.factorial(order)
    sine = sine * rest
    scale = jnp.where(wave == 0.0, jnp.sqrt(1.0 / span), jnp.sqrt(2.0 / span))
    return jnp.where((wave < span) & (place < span), (1.0 - 2.0 * sine * sine) * scale, 0.0)


def shuffle(index, side):
    half = side // 2
    return jnp.where(index < half, 2 * index, 2 * (index - half) + 1)


def layer_place(row, extent):
    return jnp.where(row < 3, row, jnp.where(row < 6, extent + 2 - row, extent))


def tables_kernel(boxes, w_ref, c_ref, ws_ref, cs_ref, ct_ref, rt_ref, sr_ref, sc_ref):
    side = w_ref.shape[1]
    spare = sr_ref.shape[1] // 6

    def paired(wave_of, place_of, length):
        shape = (2 * side, 2 * side)
        row, col = iota(shape, 0), iota(shape, 1)
        values = cosines(wave_of(row % side, col % side), place_of(row % side, col % side), length)
        return jnp.where(row // side == col // side, values, 0.0)

    def body(p, carry):
        rows, cols = boxes[p, 0], boxes[p, 1]
        shape = (side, side)
        row, col = iota(shape, 0), shuffle(iota(shape, 1), side)
        high, low = split(cosines(col, shuffle(row, side), rows))
        w_ref[p] = jnp.concatenate([high, high, low], 1)
        high, low = split(cosines(col, row, rows))
        ws_ref[p, :side] = jnp.concatenate([high, high, low], 1)
        shape = (16, side)
        row, col = iota(shape, 0), shuffle(iota(shape, 1), side)
        high, low = split(cosines(col, layer_place(row, rows), rows))
        ws_ref[p, side:] = jnp.concatenate([high, high, low], 1)
        straight = paired(lambda r, c: r, lambda r, c: c, cols)
        high, low = split(straight)
        c_ref[p] = jnp.concatenate([high, high, low], 0)
        cs_ref[p, :, : 2 * side] = jnp.concatenate([high, high, low], 0)
        shape = (2 * side, 2 * side)
        row, col = iota(shape, 0), iota(shape, 1)
        values = cosines(row % side, layer_place(col % 8, cols), cols)
        values = jnp.where((row // side == col // 8) & (col % 8 < 6), values, 0.0)
        high, low = split(values)
        cs_ref[p, :, 2 * side :] = jnp.concatenate([high, high, low], 0)
        ct_ref[p] = stacked(halves(paired(lambda r, c: c, lambda r, c: r, cols)))
        rt_ref[p] = stacked(halves(paired(lambda r, c: shuffle(c, side), lambda r, c: r, rows)))
        shape = (6 * spare, side)
        row, col = iota(shape, 0) // spare, iota(shape, 1)
        sr_ref[p] = cosines(shuffle(col, side), layer_place(row, rows), rows)
        shape = (6 * spare, 2 * side)
        row, col = iota(shape, 0) // spare, iota(shape, 1)
        sc_ref[p] = cosines(col % side, layer_place(row, cols), cols)
        return carry

    lax.fori_loop(0, w_ref.shape[0], body, 0)


def make_tables(boxes, side, spare):
    holders = boxes.shape[0]
    shapes = [
        ((holders, side, 3 * side), jnp.bfloat16),
        ((holders, 6 * side, 2 * side), jnp.bfloat16),
        ((holders, side + 16, 3 * side), jnp.bfloat16),
        ((holders, 6 * side, 4 * side), jnp.bfloat16),
        ((holders, 6 * side, 2 * side), jnp.bfloat16),
        ((holders, 6 * side, 2 * side), jnp.bfloat16),
        ((holders, 6 * spare, side), jnp.float32),
        ((holders, 6 * spare, 2 * side), jnp.float32),
    ]
    return pl.pallas_call(
        tables_kernel,
        grid_spec=pltpu.PrefetchScalarGridSpec(
            num_scalar_prefetch=1,
            grid=(1,),
            in_specs=[],
            out_specs=[whole(shape) for shape, _ in shapes],
        ),
        out_shape=[jax.ShapeDtypeStruct(*shape) for shape in shapes],
        name="tables",
        cost_estimate=pl.CostEstimate(flops=10**9, bytes_accessed=5 * 10**6, transcendentals=0),
    )(boxes)


def mix_kernel(total, chunks, spot, own_ref, other_ref, *refs):
    *out_refs, t_ref = refs
    planes, holders, step = own_ref.shape
    rows, cols = planes * holders * (len(out_refs) // chunks), 2 * planes * holders
    me = spot[0]
    masks = [m for m in range(total // planes) if m & 1 == m // (total // planes // 2)]

    @pl.when(pl.program_id(0) == 0)
    def _():
        for k, mask in enumerate(masks):
            shape = (planes * holders, cols)
            row, col = iota(shape, 0), iota(shape, 1)
            near = col < planes * holders
            mode = jnp.where(near, me * planes, (me ^ 1) * planes - planes) + col // holders
            place = (me ^ mask) * planes + row // holders
            values = jnp.where(row % holders == col % holders, cosines(mode, place, total), 0.0)
            t_ref[k * planes * holders : (k + 1) * planes * holders] = thrice(values)

    x = jnp.concatenate(
        [r[...].reshape(planes * holders, step) for r in (own_ref, other_ref)], 0
    )
    high, low = split(x)
    mixed = dot(t_ref[...], jnp.concatenate([high, high, low], 0))
    size = planes // chunks
    for k, out_ref in enumerate(out_refs):
        part = mixed[k * size * holders : (k + 1) * size * holders]
        out_ref[...] = part.reshape(size, holders, step)


def mix(spot, own, other, shares):
    planes, holders, cells = own.shape
    chunks = planes // GROUP
    count = max(1, shares // 2)
    step = min(512, cells)
    part = jax.ShapeDtypeStruct((GROUP, holders, cells), jnp.float32)
    block = lambda i, s: (0, 0, i)
    outs = pl.pallas_call(
        functools.partial(mix_kernel, shares * planes, chunks),
        grid_spec=pltpu.PrefetchScalarGridSpec(
            num_scalar_prefetch=1,
            grid=(cells // step,),
            in_specs=[pl.BlockSpec((planes, holders, step), block)] * 2,
            out_specs=[pl.BlockSpec((GROUP, holders, step), block)] * (count * chunks),
            scratch_shapes=[
                pltpu.VMEM((count * planes * holders, 6 * planes * holders), jnp.bfloat16)
            ],
        ),
        out_shape=[part] * (count * chunks),
        name="mix",
        cost_estimate=pl.CostEstimate(
            flops=3 * 10**9, bytes_accessed=16 * planes * holders * cells, transcendentals=0
        ),
    )(spot, own, other)
    return [list(outs[k * chunks : (k + 1) * chunks]) for k in range(count)]


def columns_of(planes, p, low, side):
    cols = []
    for k in range(len(planes) // 2):
        one, two = planes[2 * k][p], planes[2 * k + 1][p]
        top = jnp.where(low, one, pltpu.roll(two, side, 1))
        bottom = jnp.where(low, pltpu.roll(one, side, 1), two)
        cols.append(jnp.concatenate([top, bottom], 0))
    high, rest = split(jnp.concatenate(cols, 1))
    return jnp.concatenate([high, rest, high], 0)


def unpaired(top, bottom, low, side):
    one = jnp.where(low, top, pltpu.roll(bottom, side, 1))
    two = jnp.where(low, pltpu.roll(top, side, 1), bottom)
    return one, two


def sides_kernel(x_ref, w_ref, c_ref, s_ref):
    group, holders, cells = x_ref.shape
    side = math.isqrt(cells)
    half = side // 2
    wide = 2 * side
    low = iota((half, wide), 1) < side
    first = iota((side, wide), 1) < 8
    planes = [x_ref[z].reshape(holders, half, wide) for z in range(group)]
    pairs = group // 2
    base = pl.program_id(0) * pairs
    rows = side + 16
    for p in range(holders):
        v = dot(w_ref[p], columns_of(planes, p, low, side))
        v = jnp.concatenate([v[:, wide * k : wide * (k + 1)] for k in range(pairs)], 0)
        q = dot(thrice(v), c_ref[p])
        ends = [q[rows * k : rows * k + side, wide:] for k in range(pairs)]
        upper = jnp.where(first, ends[0], pltpu.roll(ends[1], 8, 1))
        lower = jnp.where(first, pltpu.roll(ends[0], wide - 8, 1), ends[1])
        turned = jnp.transpose(jnp.concatenate([upper, lower], 0))
        for k in range(pairs):
            for s in range(6):
                at = rows * k + side + s
                s_ref[p, s, pl.ds(base + k, 1), :] = q[at : at + 1, :wide]
                s_ref[p, 6 + s, pl.ds(base + k, 1), :] = turned[8 * k + s : 8 * k + s + 1]


def find_sides(modes, weights, columns, spare):
    planes, holders, cells = modes.shape
    wide = 2 * math.isqrt(cells)
    shape = (holders, SIDES, spare, wide)
    return pl.pallas_call(
        sides_kernel,
        grid=(planes // GROUP,),
        in_specs=[
            pl.BlockSpec((GROUP, holders, cells), lambda i: (i, 0, 0)),
            whole(weights.shape),
            whole(columns.shape),
        ],
        out_specs=whole(shape),
        out_shape=jax.ShapeDtypeStruct(shape, jnp.float32),
        name="sides",
        cost_estimate=pl.CostEstimate(
            flops=6 * 10**9, bytes_accessed=4 * planes * holders * cells, transcendentals=0
        ),
    )(modes, weights, columns)


def faces_kernel(table, s_ref, o_ref, count):
    doms, tiles, spare, wide = o_ref.shape
    slots = (tiles - 1) // 3
    place = iota((spare, wide), 1) % (wide // 2)
    lane = iota((1, wide), 1)
    o_ref[...] = jnp.zeros_like(o_ref)
    for d in range(doms):
        count[d] = 0

    def body(r, carry):
        length = table[r, 3]
        part = jnp.minimum(table[r, 0], s_ref.shape[0] - 1)
        facing = jnp.minimum(table[r, 1], 3)
        to = jnp.minimum(table[r, 4], doms - 1)
        seen = count[to]
        count[to] = seen + jnp.minimum(length, 1)
        slot = jnp.minimum(seen, slots - 1)
        for j in range(3):
            moved = pltpu.roll(s_ref[part, facing * 3 + j], wide - table[r, 2], 1)
            o_ref[to, slot * 3 + j] += jnp.where(place < length, moved, 0.0)
        label = jnp.where(lane == 0, table[r, 5], jnp.where(lane == 1, table[r, 6], table[r, 7]))
        label = jnp.where(lane == 3, length, label) * jnp.minimum(length, 1)
        o_ref[to, tiles - 1, pl.ds(slot, 1), :] += label.astype(jnp.float32)
        return carry

    lax.fori_loop(0, table.shape[0], body, 0, unroll=4)


def find_faces(sides, table, doms):
    holders, _, spare, wide = sides.shape
    slots = max(2, table.shape[0] // doms)
    shape = (doms, 3 * slots + 1, spare, wide)
    return pl.pallas_call(
        faces_kernel,
        grid_spec=pltpu.PrefetchScalarGridSpec(
            num_scalar_prefetch=1,
            grid=(1,),
            in_specs=[whole(sides.shape)],
            out_specs=whole(shape),
            scratch_shapes=[pltpu.SMEM((doms,), jnp.int32)],
        ),
        out_shape=jax.ShapeDtypeStruct(shape, jnp.float32),
        name="faces",
        cost_estimate=pl.CostEstimate(flops=10**8, bytes_accessed=10**6, transcendentals=0),
    )(table, sides)


def force_kernel(
    total, pairs, labels, spot, box_ref, r_ref, s_ref, ct_ref, rt_ref, sr_ref, sc_ref, now_ref,
    prev_ref, o_ref, f_ref, m_ref, b_ref,
):
    group, holders, cells = now_ref.shape
    doms, tiles, spare, wide = r_ref.shape
    side = wide // 2
    half = side // 2
    slots = (tiles - 1) // 3
    scale = (math.pi * TIME_STEP / 2) ** 2

    @pl.when(pl.program_id(0) == 0)
    def _():
        f_ref[...] = jnp.zeros_like(f_ref)
        place = iota((spare, wide), 1) % side

        def gather(n, carry):
            d, i = n // slots, n % slots
            part = labels[n, 0]
            facing = labels[n, 1]
            start = labels[n, 2]
            mask = (place >= start) & (place < start + labels[n, 3])
            jumps = [
                jnp.where(
                    mask,
                    pltpu.roll(r_ref[d, i * 3 + j], start, 1) - s_ref[part, facing * 3 + j],
                    0.0,
                )
                for j in range(3)
            ]
            for i in range(3):
                f_ref[part, facing * 3 + i] += sum(STENCIL[i + j] * jumps[j] for j in range(3 - i))
            return carry

        lax.fori_loop(0, doms * slots, gather, 0, unroll=4)
        shape = (6 * spare, wide)
        pair = iota(shape, 0) % spare
        left = iota(shape, 1) < side

        def spread(p, carry):
            f = f_ref[p, :6].reshape(6 * spare, wide)
            g = f_ref[p, 6:].reshape(6 * spare, wide)
            fc = dot(thrice(f), ct_ref[p])
            gr = dot(thrice(g), rt_ref[p])
            near = jnp.concatenate([sr_ref[p], gr[:, :side], gr[:, side:]], 0)
            sc = sc_ref[p]
            sc_left = jnp.where(left, sc, 0.0)
            sc_right = jnp.where(left, 0.0, sc)
            far = jnp.concatenate(
                [
                    jnp.concatenate([jnp.where(pair == k, t, 0.0) for t in (fc, sc_left, sc_right)], 0)
                    for k in range(pairs)
                ],
                1,
            )
            near_high, near_low = split(near)
            far_high, far_low = split(far)
            out = lax.dot_general(
                jnp.concatenate([near_high, near_low, near_high], 0),
                jnp.concatenate([far_high, far_high, far_low], 0),
                (((0,), (0,)), ((), ())),
                preferred_element_type=jnp.float32,
            )
            for k in range(pairs):
                m_ref[k, p] = out[:, k * wide : (k + 1) * wide]
            return carry

        lax.fori_loop(0, holders, spread, 0)
        cell = iota((holders, cells), 1)
        wave_row, wave_col = cell // side, cell % side
        extent_row, extent_col = box_ref[:, 0:1], box_ref[:, 1:2]
        ratio_row = wave_row.astype(jnp.float32) / extent_row.astype(jnp.float32)
        ratio_col = wave_col.astype(jnp.float32) / extent_col.astype(jnp.float32)
        inside = (wave_row < extent_row) & (wave_col < extent_col)
        b_ref[...] = jnp.where(inside, scale * (ratio_row * ratio_row + ratio_col * ratio_col), -1.0)

    low = iota((half, wide), 1) < side
    for k in range(group // 2):
        at = pl.program_id(0) * (group // 2) + k
        outs = [
            unpaired(m_ref[at, p, :half], m_ref[at, p, half:], low, side) for p in range(holders)
        ]
        for c in range(2):
            z = 2 * k + c
            force = jnp.stack([out[c] for out in outs], 0).reshape(holders, cells)
            depth = (spot[0] * 2 * pairs + pl.program_id(0) * group + z).astype(jnp.float32)
            depth = depth / total
            base = b_ref[...]
            quarter = base + scale * (depth * depth)
            ratio = jnp.float32(SERIES[-1])
            for coefficient in SERIES[-2::-1]:
                ratio = ratio * quarter + coefficient
            ratio = ratio * ratio
            updated = (
                (2.0 - 4.0 * quarter * ratio) * now_ref[z]
                - prev_ref[z]
                + (TIME_STEP * TIME_STEP) * ratio * force
            )
            o_ref[z] = jnp.where(base >= 0.0, updated, 0.0)


def advance(spot, boxes, received, sides, tables, modes_now, modes_prev, shares):
    planes, holders, cells = modes_now.shape
    doms, tiles, spare, wide = received.shape
    slots = (tiles - 1) // 3
    labels = received[:, tiles - 1, :slots, :4].astype(jnp.int32).reshape(doms * slots, 4)
    pairs = planes // 2
    operands = (boxes, received, sides, *tables)
    block = pl.BlockSpec((GROUP, holders, cells), lambda i, *_: (i, 0, 0))
    return pl.pallas_call(
        functools.partial(force_kernel, float(shares * planes), pairs),
        grid_spec=pltpu.PrefetchScalarGridSpec(
            num_scalar_prefetch=2,
            grid=(planes // GROUP,),
            in_specs=[whole(o.shape) for o in operands] + [block, block],
            out_specs=block,
            scratch_shapes=[
                pltpu.VMEM((holders, SIDES, spare, wide), jnp.float32),
                pltpu.VMEM((pairs, holders, wide // 2, wide), jnp.float32),
                pltpu.VMEM((holders, cells), jnp.float32),
            ],
        ),
        out_shape=jax.ShapeDtypeStruct(modes_now.shape, jnp.float32),
        name="force",
        cost_estimate=pl.CostEstimate(
            flops=8 * 10**9, bytes_accessed=12 * planes * holders * cells, transcendentals=0
        ),
    )(labels, spot, *operands, modes_now, modes_prev)


def cells_kernel(w_ref, c_ref, *refs):
    *part_refs, q_ref = [ref for ref in refs if ref is not None]
    group, holders, cells = q_ref.shape
    side = math.isqrt(cells)
    half = side // 2
    wide = 2 * side
    low = iota((half, wide), 1) < side
    planes = [sum(ref[z] for ref in part_refs).reshape(holders, half, wide) for z in range(group)]
    outs = [[] for _ in range(group)]
    for p in range(holders):
        v = dot(w_ref[p], columns_of(planes, p, low, side))
        v = jnp.concatenate([v[:, wide * k : wide * (k + 1)] for k in range(group // 2)], 0)
        q = dot(thrice(v), c_ref[p])
        for k in range(group // 2):
            pair = q[side * k : side * (k + 1)]
            outs[2 * k], outs[2 * k + 1] = (
                out + [new]
                for out, new in zip(outs[2 * k : 2 * k + 2], unpaired(pair[:half], pair[half:], low, side))
            )
    for z in range(group):
        q_ref[z] = jnp.stack(outs[z], 0).reshape(holders, cells)


def resumed_kernel(buffer_ref, *refs):
    cells_kernel(*refs)


def to_cells(parts, weights, columns, chunk, planes, buffer):
    group, holders, cells = parts[0].shape
    operands = [weights, columns, *parts]
    specs = [whole(o.shape) for o in operands]
    kernel, aliases = cells_kernel, {}
    if buffer is not None:
        operands = [buffer] + operands
        specs = [pl.BlockSpec(memory_space=pl.ANY)] + specs
        kernel, aliases = resumed_kernel, {0: 0}
    return pl.pallas_call(
        kernel,
        grid=(1,),
        in_specs=specs,
        out_specs=pl.BlockSpec((group, holders, cells), lambda i: (chunk, 0, 0)),
        out_shape=jax.ShapeDtypeStruct((planes, holders, cells), jnp.float32),
        input_output_aliases=aliases,
        name="cells",
        cost_estimate=pl.CostEstimate(
            flops=2 * 10**9, bytes_accessed=12 * group * holders * cells, transcendentals=0
        ),
    )(*operands)


def on_device(modes_now, modes_prev, partition_boxes, face_table):
    planes, holders, cells = modes_now.shape
    side = math.isqrt(cells)
    shares = lax.axis_size("height")
    doms = lax.axis_size("dom")
    spare = -(-planes // 16) * 8
    spot = lax.axis_index("height").astype(jnp.int32).reshape(1)
    masks = [m for m in range(shares) if m & 1 == m // (shares // 2)]
    swap = lambda mask: [(h, h ^ mask) for h in range(shares)]
    other = lax.ppermute(modes_now, "height", swap(1))
    w, c, ws, cs, *tables = make_tables(partition_boxes, side, spare)
    parts = mix(spot, modes_now, other, shares)
    sent = [[lax.ppermute(x, "height", swap(m)) for x in part] for m, part in zip(masks[1:], parts[1:])]
    later, _ = lax.optimization_barrier((modes_now, parts[0][0]))
    sides = find_sides(later, ws, cs, spare)
    outgoing = find_faces(sides, face_table, doms)
    received = lax.all_to_all(outgoing, "dom", split_axis=0, concat_axis=0, tiled=True)
    new_modes = advance(
        spot, partition_boxes, received, sides, tables, modes_now, modes_prev, shares
    )
    pressure = None
    parts[0][0], new_modes = lax.optimization_barrier((parts[0][0], new_modes))
    for k in range(planes // GROUP):
        pieces = [parts[0][k]] + [group[k] for group in sent]
        pressure = to_cells(pieces, w, c, k, planes, pressure)
    return (new_modes, pressure)


def solution(mesh):
    placed = (P("height", "dom", None), P("height", "dom", None), P("dom", None), P("dom", None))
    return jax.shard_map(
        on_device,
        mesh=mesh,
        in_specs=placed,
        out_specs=(P("height", "dom", None), P("height", "dom", None)),
        check_vma=False,
    )
```

```python
import functools
import math

import jax
import jax.numpy as jnp
from jax import lax
from jax.experimental import pallas as pl
from jax.experimental.pallas import tpu as pltpu
from jax.sharding import PartitionSpec as P


COUPLING = 32.0
STENCIL = (COUPLING * 270.0 / 180.0, COUPLING * -27.0 / 180.0, COUPLING * 2.0 / 180.0)
TIME_STEP = 0.4
SERIES = (1.0, -1.0 / 6, 1.0 / 120, -1.0 / 5040, 1.0 / 362880, -1.0 / 39916800, 1.0 / 6227020800)
GROUP = 4
SIDES = 12
ROOM = pltpu.CompilerParams(vmem_limit_bytes=24 * 2**20)


def iota(shape, axis):
    return lax.broadcasted_iota(jnp.int32, shape, axis)


def whole(shape):
    return pl.BlockSpec(shape, lambda *_: (0,) * len(shape))


def split(values):
    high = values.astype(jnp.bfloat16)
    return high, (values - high.astype(jnp.float32)).astype(jnp.bfloat16)


def halves(values):
    return jnp.concatenate(split(values), 0)


def dot(left, right):
    return jnp.dot(left, right, preferred_element_type=jnp.float32)


def thrice(values):
    high, low = split(values)
    return jnp.concatenate([high, low, high], 1)


def stacked(pair):
    size = pair.shape[0] // 2
    return jnp.concatenate([pair[:size], pair[:size], pair[size:]], 0)


def cosines(wave, place, length):
    span = jnp.full((1, wave.shape[1]), length, jnp.int32).astype(jnp.float32)
    inverse = 0.25 / span
    wave = wave.astype(jnp.float32)
    place = place.astype(jnp.float32)
    turns = wave * (2.0 * place + 1.0)
    rest = (turns - jnp.floor(turns * inverse + 0.5) * (4.0 * span)) * (inverse * math.pi)
    square = rest * rest
    sine = jnp.float32(1.0 / math.factorial(13))
    for order in (11, 9, 7, 5, 3, 1):
        sine = sine * square + (-1.0) ** (order // 2) / math.factorial(order)
    sine = sine * rest
    scale = jnp.where(wave == 0.0, jnp.sqrt(1.0 / span), jnp.sqrt(2.0 / span))
    return jnp.where((wave < span) & (place < span), (1.0 - 2.0 * sine * sine) * scale, 0.0)


def shuffle(index, side):
    half = side // 2
    return jnp.where(index < half, 2 * index, 2 * (index - half) + 1)


def layer_place(row, extent):
    return jnp.where(row < 3, row, jnp.where(row < 6, extent + 2 - row, extent))


def tables_kernel(boxes, w_ref, c_ref, ws_ref, cs_ref, ct_ref, rt_ref, sr_ref, sc_ref):
    side = w_ref.shape[1]
    spare = sr_ref.shape[1] // 6

    def paired(wave_of, place_of, length):
        shape = (2 * side, 2 * side)
        row, col = iota(shape, 0), iota(shape, 1)
        values = cosines(wave_of(row % side, col % side), place_of(row % side, col % side), length)
        return jnp.where(row // side == col // side, values, 0.0)

    def body(p, carry):
        rows, cols = boxes[p, 0], boxes[p, 1]
        shape = (side, side)
        row, col = iota(shape, 0), shuffle(iota(shape, 1), side)
        high, low = split(cosines(col, shuffle(row, side), rows))
        w_ref[p] = jnp.concatenate([high, high, low], 1)
        high, low = split(cosines(col, row, rows))
        ws_ref[p, :side] = jnp.concatenate([high, high, low], 1)
        shape = (16, side)
        row, col = iota(shape, 0), shuffle(iota(shape, 1), side)
        high, low = split(cosines(col, layer_place(row, rows), rows))
        ws_ref[p, side:] = jnp.concatenate([high, high, low], 1)
        straight = paired(lambda r, c: r, lambda r, c: c, cols)
        high, low = split(straight)
        c_ref[p] = jnp.concatenate([high, high, low], 0)
        cs_ref[p, :, : 2 * side] = jnp.concatenate([high, high, low], 0)
        shape = (2 * side, 2 * side)
        row, col = iota(shape, 0), iota(shape, 1)
        values = cosines(row % side, layer_place(col % 8, cols), cols)
        values = jnp.where((row // side == col // 8) & (col % 8 < 6), values, 0.0)
        high, low = split(values)
        cs_ref[p, :, 2 * side :] = jnp.concatenate([high, high, low], 0)
        ct_ref[p] = stacked(halves(paired(lambda r, c: c, lambda r, c: r, cols)))
        rt_ref[p] = stacked(halves(paired(lambda r, c: shuffle(c, side), lambda r, c: r, rows)))
        shape = (6 * spare, side)
        row, col = iota(shape, 0) // spare, iota(shape, 1)
        sr_ref[p] = cosines(shuffle(col, side), layer_place(row, rows), rows)
        shape = (6 * spare, 2 * side)
        row, col = iota(shape, 0) // spare, iota(shape, 1)
        sc_ref[p] = cosines(col % side, layer_place(row, cols), cols)
        return carry

    lax.fori_loop(0, w_ref.shape[0], body, 0)


def make_tables(boxes, side, spare):
    holders = boxes.shape[0]
    shapes = [
        ((holders, side, 3 * side), jnp.bfloat16),
        ((holders, 6 * side, 2 * side), jnp.bfloat16),
        ((holders, side + 16, 3 * side), jnp.bfloat16),
        ((holders, 6 * side, 4 * side), jnp.bfloat16),
        ((holders, 6 * side, 2 * side), jnp.bfloat16),
        ((holders, 6 * side, 2 * side), jnp.bfloat16),
        ((holders, 6 * spare, side), jnp.float32),
        ((holders, 6 * spare, 2 * side), jnp.float32),
    ]
    return pl.pallas_call(
        tables_kernel,
        grid_spec=pltpu.PrefetchScalarGridSpec(
            num_scalar_prefetch=1,
            grid=(1,),
            in_specs=[],
            out_specs=[whole(shape) for shape, _ in shapes],
        ),
        out_shape=[jax.ShapeDtypeStruct(*shape) for shape in shapes],
        name="tables",
        compiler_params=ROOM,
        cost_estimate=pl.CostEstimate(flops=10**9, bytes_accessed=5 * 10**6, transcendentals=0),
    )(boxes)


def mix_kernel(total, chunks, spot, own_ref, other_ref, *refs):
    *out_refs, t_ref = refs
    planes, holders, step = own_ref.shape
    cols = 2 * planes * holders
    me = spot[0]
    masks = [m for m in range(total // planes) if m & 1 == m // (total // planes // 2)]

    @pl.when(pl.program_id(0) == 0)
    def _():
        for k, mask in enumerate(masks):
            shape = (planes * holders, cols)
            row, col = iota(shape, 0), iota(shape, 1)
            near = col < planes * holders
            mode = jnp.where(near, me * planes, (me ^ 1) * planes - planes) + col // holders
            place = (me ^ mask) * planes + row // holders
            values = jnp.where(row % holders == col % holders, cosines(mode, place, total), 0.0)
            t_ref[k * planes * holders : (k + 1) * planes * holders] = thrice(values)

    x = jnp.concatenate(
        [r[...].reshape(planes * holders, step) for r in (own_ref, other_ref)], 0
    )
    high, low = split(x)
    mixed = dot(t_ref[...], jnp.concatenate([high, high, low], 0))
    size = planes // chunks
    for k, out_ref in enumerate(out_refs):
        part = mixed[k * size * holders : (k + 1) * size * holders]
        out_ref[...] = part.reshape(size, holders, step)


def mix(spot, own, other, shares):
    planes, holders, cells = own.shape
    chunks = planes // GROUP
    count = max(1, shares // 2)
    step = min(512, cells)
    part = jax.ShapeDtypeStruct((GROUP, holders, cells), jnp.float32)
    block = lambda i, s: (0, 0, i)
    outs = pl.pallas_call(
        functools.partial(mix_kernel, shares * planes, chunks),
        grid_spec=pltpu.PrefetchScalarGridSpec(
            num_scalar_prefetch=1,
            grid=(cells // step,),
            in_specs=[pl.BlockSpec((planes, holders, step), block)] * 2,
            out_specs=[pl.BlockSpec((GROUP, holders, step), block)] * (count * chunks),
            scratch_shapes=[
                pltpu.VMEM((count * planes * holders, 6 * planes * holders), jnp.bfloat16)
            ],
        ),
        out_shape=[part] * (count * chunks),
        name="mix",
        compiler_params=ROOM,
        cost_estimate=pl.CostEstimate(
            flops=3 * 10**9, bytes_accessed=16 * planes * holders * cells, transcendentals=0
        ),
    )(spot, own, other)
    return [list(outs[k * chunks : (k + 1) * chunks]) for k in range(count)]


def columns_of(planes, p, low, side):
    cols = []
    for k in range(len(planes) // 2):
        one, two = planes[2 * k][p], planes[2 * k + 1][p]
        top = jnp.where(low, one, pltpu.roll(two, side, 1))
        bottom = jnp.where(low, pltpu.roll(one, side, 1), two)
        cols.append(jnp.concatenate([top, bottom], 0))
    high, rest = split(jnp.concatenate(cols, 1))
    return jnp.concatenate([high, rest, high], 0)


def unpaired(top, bottom, low, side):
    one = jnp.where(low, top, pltpu.roll(bottom, side, 1))
    two = jnp.where(low, pltpu.roll(top, side, 1), bottom)
    return one, two


def sides_kernel(x_ref, w_ref, c_ref, s_ref):
    group, holders, cells = x_ref.shape
    side = math.isqrt(cells)
    half = side // 2
    wide = 2 * side
    low = iota((half, wide), 1) < side
    first = iota((side, wide), 1) < 8
    planes = [x_ref[z].reshape(holders, half, wide) for z in range(group)]
    pairs = group // 2
    base = pl.program_id(0) * pairs
    rows = side + 16
    for p in range(holders):
        v = dot(w_ref[p], columns_of(planes, p, low, side))
        v = jnp.concatenate([v[:, wide * k : wide * (k + 1)] for k in range(pairs)], 0)
        q = dot(thrice(v), c_ref[p])
        ends = [q[rows * k : rows * k + side, wide:] for k in range(pairs)]
        upper = jnp.where(first, ends[0], pltpu.roll(ends[1], 8, 1))
        lower = jnp.where(first, pltpu.roll(ends[0], wide - 8, 1), ends[1])
        turned = jnp.transpose(jnp.concatenate([upper, lower], 0))
        for k in range(pairs):
            for s in range(6):
                at = rows * k + side + s
                s_ref[p, s, pl.ds(base + k, 1), :] = q[at : at + 1, :wide]
                s_ref[p, 6 + s, pl.ds(base + k, 1), :] = turned[8 * k + s : 8 * k + s + 1]


def find_sides(modes, weights, columns, spare):
    planes, holders, cells = modes.shape
    wide = 2 * math.isqrt(cells)
    shape = (holders, SIDES, spare, wide)
    return pl.pallas_call(
        sides_kernel,
        grid=(planes // GROUP,),
        in_specs=[
            pl.BlockSpec((GROUP, holders, cells), lambda i: (i, 0, 0)),
            whole(weights.shape),
            whole(columns.shape),
        ],
        out_specs=whole(shape),
        out_shape=jax.ShapeDtypeStruct(shape, jnp.float32),
        name="sides",
        compiler_params=ROOM,
        cost_estimate=pl.CostEstimate(
            flops=6 * 10**9, bytes_accessed=4 * planes * holders * cells, transcendentals=0
        ),
    )(modes, weights, columns)


def faces_kernel(table, s_ref, o_ref, count):
    doms, tiles, spare, wide = o_ref.shape
    slots = (tiles - 1) // 3
    place = iota((spare, wide), 1) % (wide // 2)
    lane = iota((1, wide), 1)
    o_ref[...] = jnp.zeros_like(o_ref)
    for d in range(doms):
        count[d] = 0

    def body(r, carry):
        length = table[r, 3]
        part = jnp.minimum(table[r, 0], s_ref.shape[0] - 1)
        facing = jnp.minimum(table[r, 1], 3)
        to = jnp.minimum(table[r, 4], doms - 1)
        seen = count[to]
        count[to] = seen + jnp.minimum(length, 1)
        slot = jnp.minimum(seen, slots - 1)
        for j in range(3):
            moved = pltpu.roll(s_ref[part, facing * 3 + j], wide - table[r, 2], 1)
            o_ref[to, slot * 3 + j] += jnp.where(place < length, moved, 0.0)
        label = jnp.where(lane == 0, table[r, 5], jnp.where(lane == 1, table[r, 6], table[r, 7]))
        label = jnp.where(lane == 3, length, label) * jnp.minimum(length, 1)
        o_ref[to, tiles - 1, pl.ds(slot, 1), :] += label.astype(jnp.float32)
        return carry

    lax.fori_loop(0, table.shape[0], body, 0, unroll=4)


def find_faces(sides, table, doms):
    _, _, spare, wide = sides.shape
    slots = max(2, table.shape[0] // doms)
    shape = (doms, 3 * slots + 1, spare, wide)
    return pl.pallas_call(
        faces_kernel,
        grid_spec=pltpu.PrefetchScalarGridSpec(
            num_scalar_prefetch=1,
            grid=(1,),
            in_specs=[whole(sides.shape)],
            out_specs=whole(shape),
            scratch_shapes=[pltpu.SMEM((doms,), jnp.int32)],
        ),
        out_shape=jax.ShapeDtypeStruct(shape, jnp.float32),
        name="faces",
        compiler_params=ROOM,
        cost_estimate=pl.CostEstimate(flops=10**8, bytes_accessed=10**6, transcendentals=0),
    )(table, sides)


def force_kernel(
    total, pairs, labels, spot, box_ref, r_ref, s_ref, ct_ref, rt_ref, sr_ref, sc_ref, now_ref,
    prev_ref, o_ref, f_ref, m_ref, b_ref,
):
    group, holders, cells = now_ref.shape
    doms, tiles, spare, wide = r_ref.shape
    side = wide // 2
    half = side // 2
    slots = (tiles - 1) // 3
    scale = (math.pi * TIME_STEP / 2) ** 2

    @pl.when(pl.program_id(0) == 0)
    def _():
        f_ref[...] = jnp.zeros_like(f_ref)
        place = iota((spare, wide), 1) % side

        def gather(n, carry):
            d, i = n // slots, n % slots
            part = labels[n, 0]
            facing = labels[n, 1]
            start = labels[n, 2]
            mask = (place >= start) & (place < start + labels[n, 3])
            jumps = [
                jnp.where(
                    mask,
                    pltpu.roll(r_ref[d, i * 3 + j], start, 1) - s_ref[part, facing * 3 + j],
                    0.0,
                )
                for j in range(3)
            ]
            for i in range(3):
                f_ref[part, facing * 3 + i] += sum(STENCIL[i + j] * jumps[j] for j in range(3 - i))
            return carry

        lax.fori_loop(0, doms * slots, gather, 0, unroll=4)
        shape = (6 * spare, wide)
        pair = iota(shape, 0) % spare
        left = iota(shape, 1) < side

        def spread(p, carry):
            f = f_ref[p, :6].reshape(6 * spare, wide)
            g = f_ref[p, 6:].reshape(6 * spare, wide)
            fc = dot(thrice(f), ct_ref[p])
            gr = dot(thrice(g), rt_ref[p])
            near = jnp.concatenate([sr_ref[p], gr[:, :side], gr[:, side:]], 0)
            sc = sc_ref[p]
            sc_left = jnp.where(left, sc, 0.0)
            sc_right = jnp.where(left, 0.0, sc)
            far = jnp.concatenate(
                [
                    jnp.concatenate([jnp.where(pair == k, t, 0.0) for t in (fc, sc_left, sc_right)], 0)
                    for k in range(pairs)
                ],
                1,
            )
            near_high, near_low = split(near)
            far_high, far_low = split(far)
            out = lax.dot_general(
                jnp.concatenate([near_high, near_low, near_high], 0),
                jnp.concatenate([far_high, far_high, far_low], 0),
                (((0,), (0,)), ((), ())),
                preferred_element_type=jnp.float32,
            )
            for k in range(pairs):
                m_ref[k, p] = out[:, k * wide : (k + 1) * wide]
            return carry

        lax.fori_loop(0, holders, spread, 0)
        cell = iota((holders, cells), 1)
        wave_row, wave_col = cell // side, cell % side
        extent_row, extent_col = box_ref[:, 0:1], box_ref[:, 1:2]
        ratio_row = wave_row.astype(jnp.float32) / extent_row.astype(jnp.float32)
        ratio_col = wave_col.astype(jnp.float32) / extent_col.astype(jnp.float32)
        inside = (wave_row < extent_row) & (wave_col < extent_col)
        b_ref[...] = jnp.where(inside, scale * (ratio_row * ratio_row + ratio_col * ratio_col), -1.0)

    low = iota((half, wide), 1) < side
    for k in range(group // 2):
        at = pl.program_id(0) * (group // 2) + k
        outs = [
            unpaired(m_ref[at, p, :half], m_ref[at, p, half:], low, side) for p in range(holders)
        ]
        for c in range(2):
            z = 2 * k + c
            force = jnp.stack([out[c] for out in outs], 0).reshape(holders, cells)
            depth = (spot[0] * 2 * pairs + pl.program_id(0) * group + z).astype(jnp.float32)
            depth = depth / total
            base = b_ref[...]
            quarter = base + scale * (depth * depth)
            ratio = jnp.float32(SERIES[-1])
            for coefficient in SERIES[-2::-1]:
                ratio = ratio * quarter + coefficient
            ratio = ratio * ratio
            updated = (
                (2.0 - 4.0 * quarter * ratio) * now_ref[z]
                - prev_ref[z]
                + (TIME_STEP * TIME_STEP) * ratio * force
            )
            o_ref[z] = jnp.where(base >= 0.0, updated, 0.0)


def advance(spot, boxes, received, sides, tables, modes_now, modes_prev, shares):
    planes, holders, cells = modes_now.shape
    doms, tiles, spare, wide = received.shape
    slots = (tiles - 1) // 3
    labels = received[:, tiles - 1, :slots, :4].astype(jnp.int32).reshape(doms * slots, 4)
    pairs = planes // 2
    operands = (boxes, received, sides, *tables)
    block = pl.BlockSpec((GROUP, holders, cells), lambda i, *_: (i, 0, 0))
    return pl.pallas_call(
        functools.partial(force_kernel, float(shares * planes), pairs),
        grid_spec=pltpu.PrefetchScalarGridSpec(
            num_scalar_prefetch=2,
            grid=(planes // GROUP,),
            in_specs=[whole(o.shape) for o in operands] + [block, block],
            out_specs=block,
            scratch_shapes=[
                pltpu.VMEM((holders, SIDES, spare, wide), jnp.float32),
                pltpu.VMEM((pairs, holders, wide // 2, wide), jnp.float32),
                pltpu.VMEM((holders, cells), jnp.float32),
            ],
        ),
        out_shape=jax.ShapeDtypeStruct(modes_now.shape, jnp.float32),
        name="force",
        compiler_params=ROOM,
        cost_estimate=pl.CostEstimate(
            flops=8 * 10**9, bytes_accessed=12 * planes * holders * cells, transcendentals=0
        ),
    )(labels, spot, *operands, modes_now, modes_prev)


def cells_kernel(w_ref, c_ref, *refs):
    *part_refs, q_ref = [ref for ref in refs if ref is not None]
    group, holders, cells = q_ref.shape
    side = math.isqrt(cells)
    half = side // 2
    wide = 2 * side
    low = iota((half, wide), 1) < side
    planes = [sum(ref[z] for ref in part_refs).reshape(holders, half, wide) for z in range(group)]
    outs = [[] for _ in range(group)]
    for p in range(holders):
        v = dot(w_ref[p], columns_of(planes, p, low, side))
        v = jnp.concatenate([v[:, wide * k : wide * (k + 1)] for k in range(group // 2)], 0)
        q = dot(thrice(v), c_ref[p])
        for k in range(group // 2):
            pair = q[side * k : side * (k + 1)]
            outs[2 * k], outs[2 * k + 1] = (
                out + [new]
                for out, new in zip(outs[2 * k : 2 * k + 2], unpaired(pair[:half], pair[half:], low, side))
            )
    for z in range(group):
        q_ref[z] = jnp.stack(outs[z], 0).reshape(holders, cells)


def resumed_kernel(buffer_ref, *refs):
    cells_kernel(*refs)


def to_cells(parts, weights, columns, chunk, planes, buffer):
    group, holders, cells = parts[0].shape
    operands = [weights, columns, *parts]
    specs = [whole(o.shape) for o in operands]
    kernel, aliases = cells_kernel, {}
    if buffer is not None:
        operands = [buffer] + operands
        specs = [pl.BlockSpec(memory_space=pl.ANY)] + specs
        kernel, aliases = resumed_kernel, {0: 0}
    return pl.pallas_call(
        kernel,
        grid=(1,),
        in_specs=specs,
        out_specs=pl.BlockSpec((group, holders, cells), lambda i: (chunk, 0, 0)),
        out_shape=jax.ShapeDtypeStruct((planes, holders, cells), jnp.float32),
        input_output_aliases=aliases,
        name="cells",
        compiler_params=ROOM,
        cost_estimate=pl.CostEstimate(
            flops=2 * 10**9, bytes_accessed=12 * group * holders * cells, transcendentals=0
        ),
    )(*operands)


def on_device(modes_now, modes_prev, partition_boxes, face_table):
    planes, _, cells = modes_now.shape
    side = math.isqrt(cells)
    shares = lax.axis_size("height")
    doms = lax.axis_size("dom")
    spare = -(-planes // 16) * 8
    spot = lax.axis_index("height").astype(jnp.int32).reshape(1)
    masks = [m for m in range(shares) if m & 1 == m // (shares // 2)]
    swap = lambda mask: [(h, h ^ mask) for h in range(shares)]
    other = lax.ppermute(modes_now, "height", swap(1))
    w, c, ws, cs, *tables = make_tables(partition_boxes, side, spare)
    parts = mix(spot, modes_now, other, shares)
    sent = []
    for m, part in zip(masks[1:], parts[1:]):
        sent.append([lax.ppermute(x, "height", swap(m)) for x in part])
    later, _ = lax.optimization_barrier((modes_now, parts[0][0]))
    sides = find_sides(later, ws, cs, spare)
    outgoing = find_faces(sides, face_table, doms)
    received = lax.all_to_all(outgoing, "dom", split_axis=0, concat_axis=0, tiled=True)
    new_modes = advance(
        spot, partition_boxes, received, sides, tables, modes_now, modes_prev, shares
    )
    pressure = None
    parts[0][0], new_modes = lax.optimization_barrier((parts[0][0], new_modes))
    for k in range(planes // GROUP):
        pieces = [parts[0][k]] + [group[k] for group in sent]
        pressure = to_cells(pieces, w, c, k, planes, pressure)
    return (new_modes, pressure)


def solution(mesh):
    placed = (P("height", "dom", None), P("height", "dom", None), P("dom", None), P("dom", None))

    return jax.shard_map(
        on_device,
        mesh=mesh,
        in_specs=placed,
        out_specs=(P("height", "dom", None), P("height", "dom", None)),
        check_vma=False,
    )
```

```python
import functools
import math

import jax
import jax.numpy as jnp
from jax import lax
from jax.experimental import pallas as pl
from jax.experimental.pallas import tpu as pltpu
from jax.sharding import PartitionSpec as P


COUPLING = 32.0
STENCIL = (COUPLING * 270.0 / 180.0, COUPLING * -27.0 / 180.0, COUPLING * 2.0 / 180.0)
TIME_STEP = 0.4
SERIES = (1.0, -1.0 / 6, 1.0 / 120, -1.0 / 5040, 1.0 / 362880, -1.0 / 39916800, 1.0 / 6227020800)
GROUP = 4
SIDES = 12
ROOM = pltpu.CompilerParams(vmem_limit_bytes=24 * 2**20)


def iota(shape, axis):
    return lax.broadcasted_iota(jnp.int32, shape, axis)


def whole(shape):
    return pl.BlockSpec(shape, lambda *_: (0,) * len(shape))


def split(values):
    high = values.astype(jnp.bfloat16)
    return high, (values - high.astype(jnp.float32)).astype(jnp.bfloat16)


def dot(left, right):
    return jnp.dot(left, right, preferred_element_type=jnp.float32)


def thrice(values):
    high, low = split(values)
    return jnp.concatenate([high, low, high], 1)


def cosines(wave, place, length):
    span = jnp.full((1, wave.shape[1]), length, jnp.int32).astype(jnp.float32)
    inverse = 0.25 / span
    wave = wave.astype(jnp.float32)
    place = place.astype(jnp.float32)
    turns = wave * (2.0 * place + 1.0)
    rest = (turns - jnp.floor(turns * inverse + 0.5) * (4.0 * span)) * (inverse * math.pi)
    square = rest * rest
    sine = jnp.float32(1.0 / math.factorial(13))
    for order in (11, 9, 7, 5, 3, 1):
        sine = sine * square + (-1.0) ** (order // 2) / math.factorial(order)
    sine = sine * rest
    scale = jnp.where(wave == 0.0, jnp.sqrt(1.0 / span), jnp.sqrt(2.0 / span))
    return jnp.where((wave < span) & (place < span), (1.0 - 2.0 * sine * sine) * scale, 0.0)


def shuffle(index, side):
    half = side // 2
    return jnp.where(index < half, 2 * index, 2 * (index - half) + 1)


def layer_place(row, extent):
    return jnp.where(row < 3, row, jnp.where(row < 6, extent + 2 - row, extent))


def tables_kernel(boxes, faces, here, spot, w_ref, c_ref, ws_ref, cs_ref, ct_ref, rt_ref, sr_ref, sc_ref):
    side = w_ref.shape[1]
    spare = sr_ref.shape[1] // 6

    def paired(values, left):
        high, low = split(values)
        return [
            jnp.concatenate([jnp.where(left, part, 0), jnp.where(left, 0, part)], 0)
            for part in (high, high, low)
        ]

    def body(p, carry):
        rows, cols = boxes[p, 0], boxes[p, 1]
        shape = (side, side)
        row, col = iota(shape, 0), shuffle(iota(shape, 1), side)
        high, low = split(cosines(col, shuffle(row, side), rows))
        w_ref[p] = jnp.concatenate([high, high, low], 1)
        high, low = split(cosines(col, row, rows))
        ws_ref[p, :side] = jnp.concatenate([high, high, low], 1)
        shape = (16, side)
        row, col = iota(shape, 0), shuffle(iota(shape, 1), side)
        high, low = split(cosines(col, layer_place(row, rows), rows))
        ws_ref[p, side:] = jnp.concatenate([high, high, low], 1)
        shape = (side, 2 * side)
        row, wide = iota(shape, 0), iota(shape, 1)
        left, col = wide < side, wide % side
        straight = jnp.concatenate(paired(cosines(row, col, cols), left), 0)
        c_ref[p] = straight
        cs_ref[p, :, : 2 * side] = straight
        values = cosines(row, layer_place(wide % 8, cols), cols)
        values = jnp.where((wide < 16) & (wide % 8 < 6), values, 0.0)
        cs_ref[p, :, 2 * side :] = jnp.concatenate(paired(values, wide < 8), 0)
        ct_ref[p] = jnp.concatenate(paired(cosines(col, row, cols), left), 0)
        rt_ref[p] = jnp.concatenate(paired(cosines(shuffle(col, side), row, rows), left), 0)
        shape = (6 * spare, side)
        row, col = iota(shape, 0) // spare, iota(shape, 1)
        sr_ref[p] = cosines(shuffle(col, side), layer_place(row, rows), rows)
        shape = (6 * spare, 2 * side)
        row, col = iota(shape, 0) // spare, iota(shape, 1)
        sc_ref[p] = cosines(col % side, layer_place(row, cols), cols)
        return carry

    lax.fori_loop(0, w_ref.shape[0], body, 0)


def make_tables(boxes, faces, here, spot, side, spare):
    holders = boxes.shape[0]
    shapes = [
        ((holders, side, 3 * side), jnp.bfloat16),
        ((holders, 6 * side, 2 * side), jnp.bfloat16),
        ((holders, side + 16, 3 * side), jnp.bfloat16),
        ((holders, 6 * side, 4 * side), jnp.bfloat16),
        ((holders, 6 * side, 2 * side), jnp.bfloat16),
        ((holders, 6 * side, 2 * side), jnp.bfloat16),
        ((holders, 6 * spare, side), jnp.float32),
        ((holders, 6 * spare, 2 * side), jnp.float32),
    ]
    return pl.pallas_call(
        tables_kernel,
        grid_spec=pltpu.PrefetchScalarGridSpec(
            num_scalar_prefetch=4,
            grid=(1,),
            in_specs=[],
            out_specs=[whole(shape) for shape, _ in shapes],
        ),
        out_shape=[jax.ShapeDtypeStruct(*shape) for shape in shapes],
        name="tables",
        compiler_params=ROOM,
        cost_estimate=pl.CostEstimate(flops=10**9, bytes_accessed=5 * 10**6, transcendentals=0),
    )(boxes, faces, here, spot)


def mix_kernel(total, spot, own_ref, other_ref, *refs):
    *out_refs, t_ref = refs
    planes, holders, _ = own_ref.shape
    early = out_refs[0].shape[0]
    shares = total // planes
    count = planes * holders
    me = spot[0]
    masks = near_masks(shares)

    @pl.when(pl.program_id(0) == 0)
    def _():
        for k, mask in enumerate(masks):
            for odd in range(2):
                shape = (count, count)
                row, col = iota(shape, 0), iota(shape, 1)
                slot = col // holders
                half = planes // 2
                where_from = jnp.where(slot < half, me * planes, (me ^ 1) * planes - planes)
                mode = where_from + 2 * slot + odd
                place = (me ^ mask) * planes + row // holders
                values = cosines(mode, place, total)
                values = jnp.where(row % holders == col % holders, values, 0.0)
                t_ref[odd, k * count : (k + 1) * count] = thrice(values)

    mixed = []
    for odd in range(2):
        picked = [r[z] for r in (own_ref, other_ref) for z in range(odd, planes, 2)]
        high, low = split(jnp.concatenate(picked, 0))
        mixed.append(dot(t_ref[odd], jnp.concatenate([high, high, low], 0)))
    for k in range(len(masks)):
        near, far = out_refs[4 * k : 4 * k + 2], out_refs[4 * k + 2 : 4 * k + 4]
        for z in range(planes):
            at = slice((k * planes + z) * holders, (k * planes + z + 1) * holders)
            even, odd = mixed[0][at], mixed[1][at]
            for refs, n, value in ((near, z, even + odd), (far, planes - 1 - z, even - odd)):
                refs[n // early][n % early] = value


def near_masks(shares):
    top = shares // 2
    return [m for m in range(top) if m & 1 == 0]


def mix(spot, own, other, shares, front):
    planes, holders, cells = own.shape
    cells = cells - front
    count = len(near_masks(shares))
    step = math.gcd(front, cells)
    sizes = [planes - GROUP, GROUP] * (2 * count)
    block = lambda i, s: (0, 0, i)
    later = lambda i, s: (0, 0, i + front // step)
    outs = pl.pallas_call(
        functools.partial(mix_kernel, shares * planes),
        grid_spec=pltpu.PrefetchScalarGridSpec(
            num_scalar_prefetch=1,
            grid=(cells // step,),
            in_specs=[pl.BlockSpec((planes, holders, step), later)] * 2,
            out_specs=[pl.BlockSpec((size, holders, step), block) for size in sizes],
            scratch_shapes=[
                pltpu.VMEM((2, count * planes * holders, 3 * planes * holders), jnp.bfloat16)
            ],
        ),
        out_shape=[jax.ShapeDtypeStruct((size, holders, cells), jnp.float32) for size in sizes],
        name="mix",
        compiler_params=ROOM,
        cost_estimate=pl.CostEstimate(
            flops=3 * 10**9, bytes_accessed=16 * planes * holders * cells, transcendentals=0
        ),
    )(spot, own, other)
    return [list(outs[2 * k : 2 * k + 2]) for k in range(2 * count)]


def gather_kernel(places, spot, *refs):
    *in_refs, o_ref, t_ref = refs
    planes, holders, step = o_ref.shape
    count = planes * holders
    total = planes * len(places)
    me = spot[0]

    @pl.when(pl.program_id(0) == 0)
    def _():
        for k, mask in enumerate(places):
            shape = (count, count)
            row, col = iota(shape, 0), iota(shape, 1)
            values = cosines((me ^ mask) * planes + col // holders, me * planes + row // holders, total)
            high, low = split(jnp.where(row % holders == col % holders, values, 0.0))
            for n, part in enumerate((high, low, high)):
                at = n * len(places) + k
                t_ref[:, at * count : (at + 1) * count] = part

    x = jnp.concatenate([ref[...].reshape(count, step) for ref in in_refs], 0)
    high, low = split(x)
    out = dot(t_ref[...], jnp.concatenate([high, high, low], 0))
    o_ref[...] = out.reshape(planes, holders, step)


def gather_mix(spot, fields, places, front):
    planes, holders, _ = fields[0].shape
    step = front // 2
    spec = pl.BlockSpec((planes, holders, step), lambda i, s: (0, 0, i))
    count = planes * holders
    return pl.pallas_call(
        functools.partial(gather_kernel, places),
        grid_spec=pltpu.PrefetchScalarGridSpec(
            num_scalar_prefetch=1,
            grid=(front // step,),
            in_specs=[spec] * len(fields),
            out_specs=spec,
            scratch_shapes=[pltpu.VMEM((count, 3 * len(places) * count), jnp.bfloat16)],
        ),
        out_shape=jax.ShapeDtypeStruct((planes, holders, front), jnp.float32),
        name="gather",
        compiler_params=ROOM,
        cost_estimate=pl.CostEstimate(
            flops=10**9, bytes_accessed=20 * planes * holders * front, transcendentals=0
        ),
    )(spot, *fields)


def columns_of(planes, p, low, side):
    cols = []
    for k in range(len(planes) // 2):
        one, two = planes[2 * k][p], planes[2 * k + 1][p]
        top = jnp.where(low, one, pltpu.roll(two, side, 1))
        bottom = jnp.where(low, pltpu.roll(one, side, 1), two)
        cols.append(jnp.concatenate([top, bottom], 0))
    high, rest = split(jnp.concatenate(cols, 1))
    return jnp.concatenate([high, rest, high], 0)


def unpaired(top, bottom, low, side):
    one = jnp.where(low, top, pltpu.roll(bottom, side, 1))
    two = jnp.where(low, pltpu.roll(top, side, 1), bottom)
    return one, two


def sides_kernel(x_ref, w_ref, c_ref, s_ref):
    group, holders, cells = x_ref.shape
    side = math.isqrt(cells)
    half = side // 2
    wide = 2 * side
    low = iota((half, wide), 1) < side
    first = iota((side, wide), 1) < 8
    planes = [x_ref[z].reshape(holders, half, wide) for z in range(group)]
    pairs = group // 2
    base = pl.program_id(0) * pairs
    rows = side + 16
    for p in range(holders):
        v = dot(w_ref[p], columns_of(planes, p, low, side))
        v = jnp.concatenate([v[:, wide * k : wide * (k + 1)] for k in range(pairs)], 0)
        q = dot(thrice(v), c_ref[p])
        ends = [q[rows * k : rows * k + side, wide:] for k in range(pairs)]
        upper = jnp.where(first, ends[0], pltpu.roll(ends[1], 8, 1))
        lower = jnp.where(first, pltpu.roll(ends[0], wide - 8, 1), ends[1])
        turned = jnp.transpose(jnp.concatenate([upper, lower], 0))
        for k in range(pairs):
            for s in range(6):
                at = rows * k + side + s
                s_ref[p, s, pl.ds(base + k, 1), :] = q[at : at + 1, :wide]
                s_ref[p, 6 + s, pl.ds(base + k, 1), :] = turned[8 * k + s : 8 * k + s + 1]


def find_sides(modes, weights, columns, spare):
    planes, holders, cells = modes.shape
    wide = 2 * math.isqrt(cells)
    shape = (holders, SIDES, spare, wide)
    return pl.pallas_call(
        sides_kernel,
        grid=(planes // GROUP,),
        in_specs=[
            pl.BlockSpec((GROUP, holders, cells), lambda i: (i, 0, 0)),
            whole(weights.shape),
            whole(columns.shape),
        ],
        out_specs=whole(shape),
        out_shape=jax.ShapeDtypeStruct(shape, jnp.float32),
        name="sides",
        compiler_params=ROOM,
        cost_estimate=pl.CostEstimate(
            flops=6 * 10**9, bytes_accessed=4 * planes * holders * cells, transcendentals=0
        ),
    )(modes, weights, columns)


def faces_kernel(table, place_ref, s_ref, o_ref, count):
    doms, tiles, spare, wide = o_ref.shape
    slots = (tiles - 1) // 3
    place = iota((spare, wide), 1) % (wide // 2)
    lane = iota((1, wide), 1)
    o_ref[...] = jnp.zeros_like(o_ref)
    for d in range(doms):
        count[d] = 0

    def body(r, carry):
        length = table[r, 3]
        part = jnp.minimum(table[r, 0], s_ref.shape[0] - 1)
        facing = jnp.minimum(table[r, 1], 3)
        to = jnp.minimum(table[r, 4], doms - 1) ^ place_ref[0]
        seen = count[to]
        count[to] = seen + jnp.minimum(length, 1)
        slot = jnp.minimum(seen, slots - 1)
        for j in range(3):
            moved = pltpu.roll(s_ref[part, facing * 3 + j], wide - table[r, 2], 1)
            o_ref[to, slot * 3 + j] += jnp.where(place < length, moved, 0.0)
        label = jnp.where(lane == 0, table[r, 5], jnp.where(lane == 1, table[r, 6], table[r, 7]))
        label = jnp.where(lane == 3, length, label) * jnp.minimum(length, 1)
        o_ref[to, tiles - 1, pl.ds(slot, 1), :] += label.astype(jnp.float32)
        return carry

    lax.fori_loop(0, table.shape[0], body, 0, unroll=4)


def find_faces(sides, table, here, doms):
    _, _, spare, wide = sides.shape
    slots = max(2, table.shape[0] // doms)
    shape = (doms, 3 * slots + 1, spare, wide)
    return pl.pallas_call(
        faces_kernel,
        grid_spec=pltpu.PrefetchScalarGridSpec(
            num_scalar_prefetch=2,
            grid=(1,),
            in_specs=[whole(sides.shape)],
            out_specs=whole(shape),
            scratch_shapes=[pltpu.SMEM((doms,), jnp.int32)],
        ),
        out_shape=jax.ShapeDtypeStruct(shape, jnp.float32),
        name="faces",
        compiler_params=ROOM,
        cost_estimate=pl.CostEstimate(flops=10**8, bytes_accessed=10**6, transcendentals=0),
    )(table, here, sides)


def force_kernel(
    total, pairs, doms, *refs
):
    labels, spot, refs = refs[:doms], refs[doms], refs[doms + 1 :]
    box_ref, s_ref, ct_ref, rt_ref, sr_ref, sc_ref, now_ref, prev_ref, *r_refs = refs
    *r_refs, o_ref, f_ref, m_ref, b_ref = r_refs
    group, holders, cells = now_ref.shape
    tiles, spare, wide = r_refs[0].shape
    side = wide // 2
    half = side // 2
    slots = (tiles - 1) // 3
    scale = (math.pi * TIME_STEP / 2) ** 2

    @pl.when(pl.program_id(0) == 0)
    def _():
        f_ref[...] = jnp.zeros_like(f_ref)
        place = iota((spare, wide), 1) % side

        for d in range(doms):
            for n in range(slots):
                label = labels[d]
                part, facing, start = label[n, 0], label[n, 1], label[n, 2]
                mask = (place >= start) & (place < start + label[n, 3])
                jumps = []
                for j in range(3):
                    moved = pltpu.roll(r_refs[d][n * 3 + j], start, 1)
                    jumps.append(jnp.where(mask, moved - s_ref[part, facing * 3 + j], 0.0))
                for i in range(3):
                    push = sum(STENCIL[i + j] * jumps[j] for j in range(3 - i))
                    f_ref[part, facing * 3 + i] += push
        shape = (6 * spare, wide)
        pair = iota(shape, 0) % spare
        left = iota(shape, 1) < side

        def spread(p, carry):
            f = f_ref[p, :6].reshape(6 * spare, wide)
            g = f_ref[p, 6:].reshape(6 * spare, wide)
            fc = dot(thrice(f), ct_ref[p])
            gr = dot(thrice(g), rt_ref[p])
            near = jnp.concatenate([sr_ref[p], gr[:, :side], gr[:, side:]], 0)
            sc = sc_ref[p]
            sc_left = jnp.where(left, sc, 0.0)
            sc_right = jnp.where(left, 0.0, sc)
            far = jnp.concatenate(
                [
                    jnp.concatenate([jnp.where(pair == k, t, 0.0) for t in (fc, sc_left, sc_right)], 0)
                    for k in range(pairs)
                ],
                1,
            )
            near_high, near_low = split(near)
            far_high, far_low = split(far)
            out = lax.dot_general(
                jnp.concatenate([near_high, near_low, near_high], 0),
                jnp.concatenate([far_high, far_high, far_low], 0),
                (((0,), (0,)), ((), ())),
                preferred_element_type=jnp.float32,
            )
            for k in range(pairs):
                m_ref[k, p] = out[:, k * wide : (k + 1) * wide]
            return carry

        lax.fori_loop(0, holders, spread, 0)
        cell = iota((holders, cells), 1)
        wave_row, wave_col = cell // side, cell % side
        extent_row, extent_col = box_ref[:, 0:1], box_ref[:, 1:2]
        ratio_row = wave_row.astype(jnp.float32) / extent_row.astype(jnp.float32)
        ratio_col = wave_col.astype(jnp.float32) / extent_col.astype(jnp.float32)
        inside = (wave_row < extent_row) & (wave_col < extent_col)
        b_ref[...] = jnp.where(inside, scale * (ratio_row * ratio_row + ratio_col * ratio_col), -1.0)

    low = iota((half, wide), 1) < side
    for k in range(group // 2):
        at = pl.program_id(0) * (group // 2) + k
        outs = [
            unpaired(m_ref[at, p, :half], m_ref[at, p, half:], low, side) for p in range(holders)
        ]
        for c in range(2):
            z = 2 * k + c
            force = jnp.stack([out[c] for out in outs], 0).reshape(holders, cells)
            depth = (spot[0] * 2 * pairs + pl.program_id(0) * group + z).astype(jnp.float32)
            depth = depth / total
            base = b_ref[...]
            quarter = base + scale * (depth * depth)
            ratio = jnp.float32(SERIES[-1])
            for coefficient in SERIES[-2::-1]:
                ratio = ratio * quarter + coefficient
            ratio = ratio * ratio
            updated = (
                (2.0 - 4.0 * quarter * ratio) * now_ref[z]
                - prev_ref[z]
                + (TIME_STEP * TIME_STEP) * ratio * force
            )
            o_ref[z] = jnp.where(base >= 0.0, updated, 0.0)


def advance(spot, boxes, received, sides, tables, modes_now, modes_prev, shares):
    planes, holders, cells = modes_now.shape
    tiles, spare, wide = received[0].shape
    slots = (tiles - 1) // 3
    labels = [r[tiles - 1, :slots, :4].astype(jnp.int32) for r in received]
    pairs = planes // 2
    operands = (boxes, sides, *tables)
    block = pl.BlockSpec((GROUP, holders, cells), lambda i, *_: (i, 0, 0))
    return pl.pallas_call(
        functools.partial(force_kernel, float(shares * planes), pairs, len(received)),
        grid_spec=pltpu.PrefetchScalarGridSpec(
            num_scalar_prefetch=len(received) + 1,
            grid=(planes // GROUP,),
            in_specs=[whole(o.shape) for o in operands]
            + [block, block]
            + [whole(r.shape) for r in received],
            out_specs=block,
            scratch_shapes=[
                pltpu.VMEM((holders, SIDES, spare, wide), jnp.float32),
                pltpu.VMEM((pairs, holders, wide // 2, wide), jnp.float32),
                pltpu.VMEM((holders, cells), jnp.float32),
            ],
        ),
        out_shape=jax.ShapeDtypeStruct(modes_now.shape, jnp.float32),
        name="force",
        compiler_params=ROOM,
        cost_estimate=pl.CostEstimate(
            flops=8 * 10**9, bytes_accessed=12 * planes * holders * cells, transcendentals=0
        ),
    )(*labels, spot, *operands, modes_now, modes_prev, *received)


def cells_kernel(w_ref, c_ref, *refs):
    *part_refs, q_ref = [ref for ref in refs if ref is not None]
    group, holders, cells = q_ref.shape
    side = math.isqrt(cells)
    half = side // 2
    wide = 2 * side
    low = iota((half, wide), 1) < side
    first_ref, *part_refs = part_refs
    planes = []
    for z in range(group):
        rest = sum(ref[z] for ref in part_refs)
        planes.append(jnp.concatenate([first_ref[z], rest], 1).reshape(holders, half, wide))
    outs = [[] for _ in range(group)]
    for p in range(holders):
        v = dot(w_ref[p], columns_of(planes, p, low, side))
        v = jnp.concatenate([v[:, wide * k : wide * (k + 1)] for k in range(group // 2)], 0)
        q = dot(thrice(v), c_ref[p])
        for k in range(group // 2):
            pair = q[side * k : side * (k + 1)]
            outs[2 * k], outs[2 * k + 1] = (
                out + [new]
                for out, new in zip(outs[2 * k : 2 * k + 2], unpaired(pair[:half], pair[half:], low, side))
            )
    for z in range(group):
        q_ref[z] = jnp.stack(outs[z], 0).reshape(holders, cells)


def resumed_kernel(buffer_ref, *refs):
    cells_kernel(*refs)


def to_cells(first, parts, weights, columns, chunk, buffer):
    planes, holders, front = first.shape
    size, _, rest = parts[0].shape
    cells = rest + front
    operands = [weights, columns, first, *parts]
    specs = [whole(weights.shape), whole(columns.shape)]
    specs.append(pl.BlockSpec((GROUP, holders, front), lambda i: (i + chunk, 0, 0)))
    specs += [pl.BlockSpec((GROUP, holders, rest), lambda i: (i, 0, 0))] * len(parts)
    kernel, aliases = cells_kernel, {}
    if buffer is not None:
        operands = [buffer] + operands
        specs = [pl.BlockSpec(memory_space=pl.ANY)] + specs
        kernel, aliases = resumed_kernel, {0: 0}
    return pl.pallas_call(
        kernel,
        grid=(size // GROUP,),
        in_specs=specs,
        out_specs=pl.BlockSpec((GROUP, holders, cells), lambda i: (i + chunk, 0, 0)),
        out_shape=jax.ShapeDtypeStruct((planes, holders, cells), jnp.float32),
        input_output_aliases=aliases,
        name="cells",
        compiler_params=ROOM,
        cost_estimate=pl.CostEstimate(
            flops=10**8 * size * 5, bytes_accessed=12 * size * holders * cells, transcendentals=0
        ),
    )(*operands)


def on_device(modes_now, modes_prev, partition_boxes, face_table):
    planes, _, cells = modes_now.shape
    side = math.isqrt(cells)
    shares = lax.axis_size("height")
    doms = lax.axis_size("dom")
    spare = -(-planes // 16) * 8
    spot = lax.axis_index("height").astype(jnp.int32).reshape(1)
    here = lax.axis_index("dom").astype(jnp.int32).reshape(1)
    swap = lambda size, mask: [(h, h ^ mask) for h in range(size)]
    front = cells // 4
    raw, whole_modes = lax.optimization_barrier((modes_now[:, :, :front], modes_now))
    far = list(range(2, shares, 2))
    arrived = [lax.ppermute(raw, "height", swap(shares, mask)) for mask in far]
    other = lax.ppermute(whole_modes, "height", swap(shares, 1))
    w, c, ws, cs, *tables = make_tables(partition_boxes, face_table, here, spot, side, spare)
    parts = mix(spot, modes_now, other, shares, front)
    kept, sent = parts[0], [[], []]
    for k in range(2):
        for m, part in enumerate(parts[1:], 1):
            goal = near_masks(shares)[m // 2] ^ (shares - 1) * (m % 2)
            sent[k].append(lax.ppermute(part[k], "height", swap(shares, goal)))
    sides = find_sides(modes_now, ws, cs, spare)
    *arrived, sides = lax.optimization_barrier((*arrived, sides))
    passed = [lax.ppermute(x, "height", swap(shares, 1)) for x in arrived]
    outgoing = find_faces(sides, face_table, here, doms)
    received = [outgoing[0]]
    for mask in range(1, doms):
        received.append(lax.ppermute(outgoing[mask], "dom", swap(doms, mask)))
    fields = [modes_now, other, *arrived, *passed]
    places = [0, 1, *far, *(mask ^ 1 for mask in far)]
    first = gather_mix(spot, fields, places, front)
    new_modes = advance(
        spot, partition_boxes, received, sides, tables, modes_now, modes_prev, shares
    )
    pressure = None
    kept[0], new_modes = lax.optimization_barrier((kept[0], new_modes))
    for k in range(2):
        chunk = k * (planes // GROUP - 1)
        pressure = to_cells(first, [kept[k]] + sent[k], w, c, chunk, pressure)
    return (new_modes, pressure)


def solution(mesh):
    placed = (P("height", "dom", None), P("height", "dom", None), P("dom", None), P("dom", None))

    return jax.shard_map(
        on_device,
        mesh=mesh,
        in_specs=placed,
        out_specs=(P("height", "dom", None), P("height", "dom", None)),
        check_vma=False,
    )
```

```python
import functools
import math

import jax
import jax.numpy as jnp
from jax import lax
from jax.experimental import pallas as pl
from jax.experimental.pallas import tpu as pltpu
from jax.sharding import PartitionSpec as P


COUPLING = 32.0
STENCIL = (COUPLING * 270.0 / 180.0, COUPLING * -27.0 / 180.0, COUPLING * 2.0 / 180.0)
TIME_STEP = 0.4
SERIES = (1.0, -1.0 / 6, 1.0 / 120, -1.0 / 5040, 1.0 / 362880, -1.0 / 39916800)
GROUP = 4
SIDES = 12
ROOM = pltpu.CompilerParams(vmem_limit_bytes=24 * 2**20)


def iota(shape, axis):
    return lax.broadcasted_iota(jnp.int32, shape, axis)


def whole(shape):
    return pl.BlockSpec(shape, lambda *_: (0,) * len(shape))


def split(values):
    high = values.astype(jnp.bfloat16)
    return high, (values - high.astype(jnp.float32)).astype(jnp.bfloat16)


def dot(left, right):
    return jnp.dot(left, right, preferred_element_type=jnp.float32)


def thrice(values):
    high, low = split(values)
    return jnp.concatenate([high, low, high], 1)


def cosines(wave, place, length):
    span = jnp.full((1, wave.shape[1]), length, jnp.int32).astype(jnp.float32)
    inverse = 0.25 / span
    wave = wave.astype(jnp.float32)
    place = place.astype(jnp.float32)
    turns = wave * (2.0 * place + 1.0)
    rest = (turns - jnp.floor(turns * inverse + 0.5) * (4.0 * span)) * (inverse * math.pi)
    square = rest * rest
    sine = jnp.float32(1.0 / math.factorial(13))
    for order in (11, 9, 7, 5, 3, 1):
        sine = sine * square + (-1.0) ** (order // 2) / math.factorial(order)
    sine = sine * rest
    scale = jnp.where(wave == 0.0, jnp.sqrt(1.0 / span), jnp.sqrt(2.0 / span))
    return jnp.where((wave < span) & (place < span), (1.0 - 2.0 * sine * sine) * scale, 0.0)


def shuffle(index, side):
    half = side // 2
    return jnp.where(index < half, 2 * index, 2 * (index - half) + 1)


def layer_place(row, extent):
    return jnp.where(row < 3, row, jnp.where(row < 6, extent + 2 - row, extent))


def tables_kernel(boxes, faces, here, spot, w_ref, c_ref, ws_ref, cs_ref, ct_ref, rt_ref, sr_ref, sc_ref):
    side = w_ref.shape[1]
    spare = sr_ref.shape[1] // 6

    def paired(values, left):
        high, low = split(values)
        return [
            jnp.concatenate([jnp.where(left, part, 0), jnp.where(left, 0, part)], 0)
            for part in (high, high, low)
        ]

    def body(p, carry):
        rows, cols = boxes[p, 0], boxes[p, 1]
        shape = (side, side)
        row, col = iota(shape, 0), shuffle(iota(shape, 1), side)
        high, low = split(cosines(col, shuffle(row, side), rows))
        w_ref[p] = jnp.concatenate([high, high, low], 1)
        high, low = split(cosines(col, row, rows))
        ws_ref[p, :side] = jnp.concatenate([high, high, low], 1)
        shape = (16, side)
        row, col = iota(shape, 0), shuffle(iota(shape, 1), side)
        high, low = split(cosines(col, layer_place(row, rows), rows))
        ws_ref[p, side:] = jnp.concatenate([high, high, low], 1)
        shape = (side, 2 * side)
        row, wide = iota(shape, 0), iota(shape, 1)
        left, col = wide < side, wide % side
        straight = jnp.concatenate(paired(cosines(row, col, cols), left), 0)
        c_ref[p] = straight
        cs_ref[p, :, : 2 * side] = straight
        values = cosines(row, layer_place(wide % 8, cols), cols)
        values = jnp.where((wide < 16) & (wide % 8 < 6), values, 0.0)
        cs_ref[p, :, 2 * side :] = jnp.concatenate(paired(values, wide < 8), 0)
        ct_ref[p] = jnp.concatenate(paired(cosines(col, row, cols), left), 0)
        rt_ref[p] = jnp.concatenate(paired(cosines(shuffle(col, side), row, rows), left), 0)
        shape = (6 * spare, side)
        row, col = iota(shape, 0) // spare, iota(shape, 1)
        sr_ref[p] = cosines(shuffle(col, side), layer_place(row, rows), rows)
        shape = (6 * spare, 2 * side)
        row, col = iota(shape, 0) // spare, iota(shape, 1)
        sc_ref[p] = cosines(col % side, layer_place(row, cols), cols)
        return carry

    lax.fori_loop(0, w_ref.shape[0], body, 0)


def make_tables(boxes, faces, here, spot, side, spare):
    holders = boxes.shape[0]
    shapes = [
        ((holders, side, 3 * side), jnp.bfloat16),
        ((holders, 6 * side, 2 * side), jnp.bfloat16),
        ((holders, side + 16, 3 * side), jnp.bfloat16),
        ((holders, 6 * side, 4 * side), jnp.bfloat16),
        ((holders, 6 * side, 2 * side), jnp.bfloat16),
        ((holders, 6 * side, 2 * side), jnp.bfloat16),
        ((holders, 6 * spare, side), jnp.float32),
        ((holders, 6 * spare, 2 * side), jnp.float32),
    ]
    return pl.pallas_call(
        tables_kernel,
        grid_spec=pltpu.PrefetchScalarGridSpec(
            num_scalar_prefetch=4,
            grid=(1,),
            in_specs=[],
            out_specs=[whole(shape) for shape, _ in shapes],
        ),
        out_shape=[jax.ShapeDtypeStruct(*shape) for shape in shapes],
        name="tables",
        compiler_params=ROOM,
        cost_estimate=pl.CostEstimate(flops=10**9, bytes_accessed=5 * 10**6, transcendentals=0),
    )(boxes, faces, here, spot)


def mix_kernel(total, spot, own_ref, other_ref, *refs):
    *out_refs, t_ref = refs
    planes, holders, _ = own_ref.shape
    early = out_refs[0].shape[0]
    shares = total // planes
    count = planes * holders
    me = spot[0]
    masks = near_masks(shares)

    @pl.when(pl.program_id(0) == 0)
    def _():
        for k, mask in enumerate(masks):
            for odd in range(2):
                shape = (count, count)
                row, col = iota(shape, 0), iota(shape, 1)
                slot = col // holders
                half = planes // 2
                where_from = jnp.where(slot < half, me * planes, (me ^ 1) * planes - planes)
                mode = where_from + 2 * slot + odd
                place = (me ^ mask) * planes + row // holders
                values = cosines(mode, place, total)
                values = jnp.where(row % holders == col % holders, values, 0.0)
                t_ref[odd, k * count : (k + 1) * count] = thrice(values)

    mixed = []
    for odd in range(2):
        picked = [r[z] for r in (own_ref, other_ref) for z in range(odd, planes, 2)]
        high, low = split(jnp.concatenate(picked, 0))
        mixed.append(dot(t_ref[odd], jnp.concatenate([high, high, low], 0)))
    for k in range(len(masks)):
        near, far = out_refs[4 * k : 4 * k + 2], out_refs[4 * k + 2 : 4 * k + 4]
        for z in range(planes):
            at = slice((k * planes + z) * holders, (k * planes + z + 1) * holders)
            even, odd = mixed[0][at], mixed[1][at]
            for refs, n, value in ((near, z, even + odd), (far, planes - 1 - z, even - odd)):
                refs[n // early][n % early] = value


def near_masks(shares):
    top = shares // 2
    return [m for m in range(top) if m & 1 == 0]


def mix(spot, own, other, shares, front):
    planes, holders, cells = own.shape
    cells = cells - front
    count = len(near_masks(shares))
    step = math.gcd(front, cells)
    sizes = [planes - GROUP, GROUP] * (2 * count)
    block = lambda i, s: (0, 0, i)
    later = lambda i, s: (0, 0, i + front // step)
    outs = pl.pallas_call(
        functools.partial(mix_kernel, shares * planes),
        grid_spec=pltpu.PrefetchScalarGridSpec(
            num_scalar_prefetch=1,
            grid=(cells // step,),
            in_specs=[pl.BlockSpec((planes, holders, step), later)] * 2,
            out_specs=[pl.BlockSpec((size, holders, step), block) for size in sizes],
            scratch_shapes=[
                pltpu.VMEM((2, count * planes * holders, 3 * planes * holders), jnp.bfloat16)
            ],
        ),
        out_shape=[jax.ShapeDtypeStruct((size, holders, cells), jnp.float32) for size in sizes],
        name="mix",
        compiler_params=ROOM,
        cost_estimate=pl.CostEstimate(
            flops=3 * 10**9, bytes_accessed=16 * planes * holders * cells, transcendentals=0
        ),
    )(spot, own, other)
    return [list(outs[2 * k : 2 * k + 2]) for k in range(2 * count)]


def exchange_kernel(total, places, box_ref, out_ref, now_ref, prev_ref, *refs):
    field_refs = refs[: len(places)]
    r_ref, first_ref, kept_ref, gain_ref, land_ref, t_ref, send_sem, recv_sem = refs[len(places) :]
    doms = out_ref.shape[0]
    planes, holders, cells = now_ref.shape
    front = first_ref.shape[2]
    here = lax.axis_index("dom")
    me = lax.axis_index("height")
    count = planes * holders

    barrier = pltpu.get_barrier_semaphore()
    for m in range(1, doms):
        goal = {"dom": lax.rem(here + m, doms)}
        pl.semaphore_signal(barrier, inc=1, device_id=goal, device_id_type=pl.DeviceIdType.MESH)
    for k, mask in enumerate(places):
        shape = (count, count)
        row, col = iota(shape, 0), iota(shape, 1)
        values = cosines((me ^ mask) * planes + col // holders, me * planes + row // holders, total)
        high, low = split(jnp.where(row % holders == col % holders, values, 0.0))
        for n, part in enumerate((high, low, high)):
            at = n * len(places) + k
            t_ref[:, at * count : (at + 1) * count] = part
    pl.semaphore_wait(barrier, doms - 1)
    copies = []
    for m in range(1, doms):
        copy = pltpu.make_async_remote_copy(
            src_ref=out_ref.at[m],
            dst_ref=land_ref.at[m],
            send_sem=send_sem.at[m],
            recv_sem=recv_sem.at[m],
            device_id={"dom": lax.rem(here + m, doms)},
            device_id_type=pl.DeviceIdType.MESH,
        )
        copy.start()
        copies.append(copy)
    r_ref[0] = out_ref[0]

    step = front // 4
    for n in range(4):
        at = slice(n * step, (n + 1) * step)
        x = jnp.concatenate([ref[:, :, at].reshape(count, step) for ref in field_refs], 0)
        high, low = split(x)
        mixed = dot(t_ref[...], jnp.concatenate([high, high, low], 0))
        first_ref[:, :, at] = mixed.reshape(planes, holders, step)

    scale = (math.pi * TIME_STEP / 2) ** 2
    side = math.isqrt(cells)
    cell = iota((holders, cells), 1)
    wave_row, wave_col = cell // side, cell % side
    extent_row, extent_col = box_ref[:, 0:1], box_ref[:, 1:2]
    ratio_row = wave_row.astype(jnp.float32) / extent_row.astype(jnp.float32)
    ratio_col = wave_col.astype(jnp.float32) / extent_col.astype(jnp.float32)
    inside = (wave_row < extent_row) & (wave_col < extent_col)
    base = scale * (ratio_row * ratio_row + ratio_col * ratio_col)
    gain_ref[0] = jnp.where(inside, base, -1.0)
    kept_ref[0] = jnp.where(inside, base, -1.0)

    def pace(n, carry):
        z = planes - 1 - n
        base = gain_ref[0]
        depth = (me * planes + z).astype(jnp.float32) / total
        quarter = base + scale * (depth * depth)
        ratio = jnp.float32(SERIES[-1])
        for coefficient in SERIES[-2::-1]:
            ratio = ratio * quarter + coefficient
        ratio = ratio * ratio
        kept = (2.0 - 4.0 * quarter * ratio) * now_ref[z] - prev_ref[z]
        kept_ref[z] = jnp.where(base >= 0.0, kept, 0.0)
        gain_ref[z] = jnp.where(base >= 0.0, (TIME_STEP * TIME_STEP) * ratio, 0.0)
        return carry

    lax.fori_loop(0, planes, pace, 0)
    for copy in copies:
        copy.wait_recv()
    for m in range(1, doms):
        r_ref[m] = land_ref[m]
    for copy in copies:
        copy.wait_send()


def exchange(boxes, outgoing, now, prev, fields, places, front, shares):
    planes, holders, _ = now.shape
    count = planes * holders
    doms = outgoing.shape[0]
    field = pl.BlockSpec((planes, holders, front), lambda i: (0, 0, 0))
    like = lambda shape: jax.ShapeDtypeStruct(shape, jnp.float32)
    outs = [outgoing.shape, (planes, holders, front), now.shape, now.shape]
    return pl.pallas_call(
        functools.partial(exchange_kernel, shares * planes, places),
        grid=(1,),
        in_specs=[whole(o.shape) for o in (boxes, outgoing, now, prev)] + [field] * len(fields),
        out_specs=[whole(shape) for shape in outs],
        out_shape=[like(shape) for shape in outs],
        scratch_shapes=[
            pltpu.VMEM(outgoing.shape, jnp.float32),
            pltpu.VMEM((count, 3 * len(places) * count), jnp.bfloat16),
            pltpu.SemaphoreType.DMA((doms,)),
            pltpu.SemaphoreType.DMA((doms,)),
        ],
        name="exchange",
        compiler_params=pltpu.CompilerParams(
            vmem_limit_bytes=24 * 2**20, collective_id=0, has_side_effects=True
        ),
        cost_estimate=pl.CostEstimate(
            flops=10**10, bytes_accessed=20 * planes * holders * front, transcendentals=0
        ),
    )(boxes, outgoing, now, prev, *fields)


def columns_of(planes, p, low, side):
    cols = []
    for k in range(len(planes) // 2):
        one, two = planes[2 * k][p], planes[2 * k + 1][p]
        top = jnp.where(low, one, pltpu.roll(two, side, 1))
        bottom = jnp.where(low, pltpu.roll(one, side, 1), two)
        cols.append(jnp.concatenate([top, bottom], 0))
    high, rest = split(jnp.concatenate(cols, 1))
    return jnp.concatenate([high, rest, high], 0)


def unpaired(top, bottom, low, side):
    one = jnp.where(low, top, pltpu.roll(bottom, side, 1))
    two = jnp.where(low, pltpu.roll(top, side, 1), bottom)
    return one, two


def sides_kernel(x_ref, w_ref, c_ref, s_ref):
    group, holders, cells = x_ref.shape
    side = math.isqrt(cells)
    half = side // 2
    wide = 2 * side
    low = iota((half, wide), 1) < side
    first = iota((side, wide), 1) < 8
    planes = [x_ref[z].reshape(holders, half, wide) for z in range(group)]
    pairs = group // 2
    base = pl.program_id(0) * pairs
    rows = side + 16
    for p in range(holders):
        v = dot(w_ref[p], columns_of(planes, p, low, side))
        v = jnp.concatenate([v[:, wide * k : wide * (k + 1)] for k in range(pairs)], 0)
        q = dot(thrice(v), c_ref[p])
        ends = [q[rows * k : rows * k + side, wide:] for k in range(pairs)]
        upper = jnp.where(first, ends[0], pltpu.roll(ends[1], 8, 1))
        lower = jnp.where(first, pltpu.roll(ends[0], wide - 8, 1), ends[1])
        turned = jnp.transpose(jnp.concatenate([upper, lower], 0))
        for k in range(pairs):
            for s in range(6):
                at = rows * k + side + s
                s_ref[p, s, pl.ds(base + k, 1), :] = q[at : at + 1, :wide]
                s_ref[p, 6 + s, pl.ds(base + k, 1), :] = turned[8 * k + s : 8 * k + s + 1]


def find_sides(modes, weights, columns, spare):
    planes, holders, cells = modes.shape
    wide = 2 * math.isqrt(cells)
    shape = (holders, SIDES, spare, wide)
    return pl.pallas_call(
        sides_kernel,
        grid=(planes // GROUP,),
        in_specs=[
            pl.BlockSpec((GROUP, holders, cells), lambda i: (i, 0, 0)),
            whole(weights.shape),
            whole(columns.shape),
        ],
        out_specs=whole(shape),
        out_shape=jax.ShapeDtypeStruct(shape, jnp.float32),
        name="sides",
        compiler_params=ROOM,
        cost_estimate=pl.CostEstimate(
            flops=6 * 10**9, bytes_accessed=4 * planes * holders * cells, transcendentals=0
        ),
    )(modes, weights, columns)


def faces_kernel(table, place_ref, s_ref, o_ref, count):
    doms, tiles, spare, wide = o_ref.shape
    slots = (tiles - 1) // 3
    place = iota((spare, wide), 1) % (wide // 2)
    lane = iota((1, wide), 1)
    o_ref[...] = jnp.zeros_like(o_ref)
    for d in range(doms):
        count[d] = 0

    def body(r, carry):
        length = table[r, 3]
        part = jnp.minimum(table[r, 0], s_ref.shape[0] - 1)
        facing = jnp.minimum(table[r, 1], 3)
        to = jnp.minimum(table[r, 4], doms - 1) - place_ref[0]
        to = jnp.where(to < 0, to + doms, to)
        seen = count[to]
        count[to] = seen + jnp.minimum(length, 1)
        slot = jnp.minimum(seen, slots - 1)
        for j in range(3):
            moved = pltpu.roll(s_ref[part, facing * 3 + j], wide - table[r, 2], 1)
            o_ref[to, slot * 3 + j] += jnp.where(place < length, moved, 0.0)
        label = jnp.where(lane == 0, table[r, 5], jnp.where(lane == 1, table[r, 6], table[r, 7]))
        label = jnp.where(lane == 3, length, label) * jnp.minimum(length, 1)
        o_ref[to, tiles - 1, pl.ds(slot, 1), :] += label.astype(jnp.float32)
        return carry

    lax.fori_loop(0, table.shape[0], body, 0, unroll=4)


def find_faces(sides, table, here, doms):
    _, _, spare, wide = sides.shape
    slots = max(2, table.shape[0] // doms)
    shape = (doms, 3 * slots + 1, spare, wide)
    return pl.pallas_call(
        faces_kernel,
        grid_spec=pltpu.PrefetchScalarGridSpec(
            num_scalar_prefetch=2,
            grid=(1,),
            in_specs=[whole(sides.shape)],
            out_specs=whole(shape),
            scratch_shapes=[pltpu.SMEM((doms,), jnp.int32)],
        ),
        out_shape=jax.ShapeDtypeStruct(shape, jnp.float32),
        name="faces",
        compiler_params=ROOM,
        cost_estimate=pl.CostEstimate(flops=10**8, bytes_accessed=10**6, transcendentals=0),
    )(table, here, sides)


def force_kernel(
    pairs, labels, r_ref, s_ref, ct_ref, rt_ref, sr_ref, sc_ref, kept_ref, gain_ref, o_ref, f_ref,
    m_ref,
):
    group, holders, cells = kept_ref.shape
    doms, tiles, spare, wide = r_ref.shape
    side = wide // 2
    half = side // 2
    slots = (tiles - 1) // 3

    @pl.when(pl.program_id(0) == 0)
    def _():
        f_ref[...] = jnp.zeros_like(f_ref)
        place = iota((spare, wide), 1) % side

        for d in range(doms):
            for n in range(slots):
                at = d * slots + n
                part, facing, start = labels[at, 0], labels[at, 1], labels[at, 2]
                mask = (place >= start) & (place < start + labels[at, 3])
                jumps = []
                for j in range(3):
                    moved = pltpu.roll(r_ref[d, n * 3 + j], start, 1)
                    jumps.append(jnp.where(mask, moved - s_ref[part, facing * 3 + j], 0.0))
                for i in range(3):
                    push = sum(STENCIL[i + j] * jumps[j] for j in range(3 - i))
                    f_ref[part, facing * 3 + i] += push
        shape = (6 * spare, wide)
        pair = iota(shape, 0) % spare
        left = iota(shape, 1) < side

        def spread(p, carry):
            f = f_ref[p, :6].reshape(6 * spare, wide)
            g = f_ref[p, 6:].reshape(6 * spare, wide)
            fc = dot(thrice(f), ct_ref[p])
            gr = dot(thrice(g), rt_ref[p])
            near = jnp.concatenate([sr_ref[p], gr[:, :side], gr[:, side:]], 0)
            sc = sc_ref[p]
            sc_left = jnp.where(left, sc, 0.0)
            sc_right = jnp.where(left, 0.0, sc)
            highs, lows = zip(*(split(t) for t in (fc, sc_left, sc_right)))
            masks = [jnp.where(pair == k, 1.0, 0.0).astype(jnp.bfloat16) for k in range(pairs)]
            far_high, far_low = (
                jnp.concatenate(
                    [jnp.concatenate([t * mask for t in parts], 0) for mask in masks], 1
                )
                for parts in (highs, lows)
            )
            near_high, near_low = split(near)
            out = lax.dot_general(
                jnp.concatenate([near_high, near_low, near_high], 0),
                jnp.concatenate([far_high, far_high, far_low], 0),
                (((0,), (0,)), ((), ())),
                preferred_element_type=jnp.float32,
            )
            for k in range(pairs):
                m_ref[k, p] = out[:, k * wide : (k + 1) * wide]
            return carry

        lax.fori_loop(0, holders, spread, 0)

    low = iota((half, wide), 1) < side
    for k in range(group // 2):
        at = pl.program_id(0) * (group // 2) + k
        outs = [
            unpaired(m_ref[at, p, :half], m_ref[at, p, half:], low, side) for p in range(holders)
        ]
        for c in range(2):
            z = 2 * k + c
            force = jnp.stack([out[c] for out in outs], 0).reshape(holders, cells)
            o_ref[z] = kept_ref[z] + gain_ref[z] * force


def advance(received, sides, tables, kept, gain):
    planes, holders, cells = kept.shape
    doms, tiles, spare, wide = received.shape
    slots = (tiles - 1) // 3
    labels = received[:, tiles - 1, :slots, :4].astype(jnp.int32).reshape(doms * slots, 4)
    pairs = planes // 2
    operands = (received, sides, *tables)
    block = pl.BlockSpec((GROUP, holders, cells), lambda i, *_: (i, 0, 0))
    return pl.pallas_call(
        functools.partial(force_kernel, pairs),
        grid_spec=pltpu.PrefetchScalarGridSpec(
            num_scalar_prefetch=1,
            grid=(planes // GROUP,),
            in_specs=[whole(o.shape) for o in operands] + [block, block],
            out_specs=block,
            scratch_shapes=[
                pltpu.VMEM((holders, SIDES, spare, wide), jnp.float32),
                pltpu.VMEM((pairs, holders, wide // 2, wide), jnp.float32),
            ],
        ),
        out_shape=jax.ShapeDtypeStruct(kept.shape, jnp.float32),
        name="force",
        compiler_params=ROOM,
        cost_estimate=pl.CostEstimate(
            flops=8 * 10**9, bytes_accessed=12 * planes * holders * cells, transcendentals=0
        ),
    )(labels, *operands, kept, gain)


def cells_kernel(w_ref, c_ref, *refs):
    *part_refs, q_ref = [ref for ref in refs if ref is not None]
    group, holders, cells = q_ref.shape
    side = math.isqrt(cells)
    half = side // 2
    wide = 2 * side
    low = iota((half, wide), 1) < side
    first_ref, *part_refs = part_refs
    planes = []
    for z in range(group):
        rest = sum(ref[z] for ref in part_refs)
        planes.append(jnp.concatenate([first_ref[z], rest], 1).reshape(holders, half, wide))
    outs = [[] for _ in range(group)]
    for p in range(holders):
        v = dot(w_ref[p], columns_of(planes, p, low, side))
        v = jnp.concatenate([v[:, wide * k : wide * (k + 1)] for k in range(group // 2)], 0)
        q = dot(thrice(v), c_ref[p])
        for k in range(group // 2):
            pair = q[side * k : side * (k + 1)]
            outs[2 * k], outs[2 * k + 1] = (
                out + [new]
                for out, new in zip(outs[2 * k : 2 * k + 2], unpaired(pair[:half], pair[half:], low, side))
            )
    for z in range(group):
        q_ref[z] = jnp.stack(outs[z], 0).reshape(holders, cells)


def resumed_kernel(buffer_ref, *refs):
    cells_kernel(*refs)


def to_cells(first, parts, weights, columns, chunk, buffer):
    planes, holders, front = first.shape
    size, _, rest = parts[0].shape
    cells = rest + front
    operands = [weights, columns, first, *parts]
    specs = [whole(weights.shape), whole(columns.shape)]
    specs.append(pl.BlockSpec((GROUP, holders, front), lambda i: (i + chunk, 0, 0)))
    specs += [pl.BlockSpec((GROUP, holders, rest), lambda i: (i, 0, 0))] * len(parts)
    kernel, aliases = cells_kernel, {}
    if buffer is not None:
        operands = [buffer] + operands
        specs = [pl.BlockSpec(memory_space=pl.ANY)] + specs
        kernel, aliases = resumed_kernel, {0: 0}
    return pl.pallas_call(
        kernel,
        grid=(size // GROUP,),
        in_specs=specs,
        out_specs=pl.BlockSpec((GROUP, holders, cells), lambda i: (i + chunk, 0, 0)),
        out_shape=jax.ShapeDtypeStruct((planes, holders, cells), jnp.float32),
        input_output_aliases=aliases,
        name="cells",
        compiler_params=ROOM,
        cost_estimate=pl.CostEstimate(
            flops=10**8 * size * 5, bytes_accessed=12 * size * holders * cells, transcendentals=0
        ),
    )(*operands)


def on_device(modes_now, modes_prev, partition_boxes, face_table):
    planes, _, cells = modes_now.shape
    side = math.isqrt(cells)
    shares = lax.axis_size("height")
    doms = lax.axis_size("dom")
    spare = -(-planes // 16) * 8
    spot = lax.axis_index("height").astype(jnp.int32).reshape(1)
    here = lax.axis_index("dom").astype(jnp.int32).reshape(1)
    swap = lambda size, mask: [(h, h ^ mask) for h in range(size)]
    front = cells // 4
    raw, whole_modes = lax.optimization_barrier((modes_now[:, :, :front], modes_now))
    far = list(range(2, shares, 2))
    arrived = [lax.ppermute(raw, "height", swap(shares, mask)) for mask in far]
    other = lax.ppermute(whole_modes, "height", swap(shares, 1))
    w, c, ws, cs, *tables = make_tables(partition_boxes, face_table, here, spot, side, spare)
    parts = mix(spot, modes_now, other, shares, front)
    kept, sent = parts[0], [[], []]
    for k in range(2):
        for m, part in enumerate(parts[1:], 1):
            goal = near_masks(shares)[m // 2] ^ (shares - 1) * (m % 2)
            sent[k].append(lax.ppermute(part[k], "height", swap(shares, goal)))
    sides = find_sides(modes_now, ws, cs, spare)
    *arrived, sides = lax.optimization_barrier((*arrived, sides))
    passed = [lax.ppermute(x, "height", swap(shares, 1)) for x in arrived]
    outgoing = find_faces(sides, face_table, here, doms)
    fields = [modes_now, other, *arrived, *passed]
    places = [0, 1, *far, *(mask ^ 1 for mask in far)]
    received, first, steady, gain = exchange(
        partition_boxes, outgoing, modes_now, modes_prev, fields, places, front, shares
    )
    new_modes = advance(received, sides, tables, steady, gain)
    pressure = None
    kept[0], new_modes = lax.optimization_barrier((kept[0], new_modes))
    for k in range(2):
        chunk = k * (planes // GROUP - 1)
        pressure = to_cells(first, [kept[k]] + sent[k], w, c, chunk, pressure)
    return (new_modes, pressure)


def solution(mesh):
    placed = (P("height", "dom", None), P("height", "dom", None), P("dom", None), P("dom", None))

    return jax.shard_map(
        on_device,
        mesh=mesh,
        in_specs=placed,
        out_specs=(P("height", "dom", None), P("height", "dom", None)),
        check_vma=False,
    )
```

```python
import functools
import math

import jax
import jax.numpy as jnp
from jax import lax
from jax.experimental import pallas as pl
from jax.experimental.pallas import tpu as pltpu
from jax.sharding import PartitionSpec as P


COUPLING = 32.0
STENCIL = (COUPLING * 270.0 / 180.0, COUPLING * -27.0 / 180.0, COUPLING * 2.0 / 180.0)
TIME_STEP = 0.4
SERIES = (1.0, -1.0 / 6, 1.0 / 120, -1.0 / 5040, 1.0 / 362880, -1.0 / 39916800)
GROUP = 4
SIDES = 12
ROOM = pltpu.CompilerParams(vmem_limit_bytes=24 * 2**20)


def iota(shape, axis):
    return lax.broadcasted_iota(jnp.int32, shape, axis)


def whole(shape):
    return pl.BlockSpec(shape, lambda *_: (0,) * len(shape))


def split(values):
    high = values.astype(jnp.bfloat16)
    return high, (values - high.astype(jnp.float32)).astype(jnp.bfloat16)


def dot(left, right):
    return jnp.dot(left, right, preferred_element_type=jnp.float32)


def thrice(values):
    high, low = split(values)
    return jnp.concatenate([high, low, high], 1)


def cosines(wave, place, length):
    span = jnp.full((1, wave.shape[1]), length, jnp.int32).astype(jnp.float32)
    inverse = 0.25 / span
    wave = wave.astype(jnp.float32)
    place = place.astype(jnp.float32)
    turns = wave * (2.0 * place + 1.0)
    rest = (turns - jnp.floor(turns * inverse + 0.5) * (4.0 * span)) * (inverse * math.pi)
    square = rest * rest
    sine = jnp.float32(1.0 / math.factorial(13))
    for order in (11, 9, 7, 5, 3, 1):
        sine = sine * square + (-1.0) ** (order // 2) / math.factorial(order)
    sine = sine * rest
    scale = jnp.where(wave == 0.0, jnp.sqrt(1.0 / span), jnp.sqrt(2.0 / span))
    return jnp.where((wave < span) & (place < span), (1.0 - 2.0 * sine * sine) * scale, 0.0)


def shuffle(index, side):
    half = side // 2
    return jnp.where(index < half, 2 * index, 2 * (index - half) + 1)


def layer_place(row, extent):
    return jnp.where(row < 3, row, jnp.where(row < 6, extent + 2 - row, extent))


def paired(values, left):
    high, low = split(values)
    return [
        jnp.concatenate([jnp.where(left, part, 0), jnp.where(left, 0, part)], 0)
        for part in (high, high, low)
    ]


def force_tables(p, boxes, ct_ref, rt_ref, sr_ref, sc_ref):
    rows, cols = boxes[0, p], boxes[1, p]
    side = sr_ref.shape[2]
    spare = sr_ref.shape[1] // 6
    shape = (side, 2 * side)
    row, wide = iota(shape, 0), iota(shape, 1)
    left, col = wide < side, wide % side
    ct_ref[p] = jnp.concatenate(paired(cosines(col, row, cols), left), 0)
    rt_ref[p] = jnp.concatenate(paired(cosines(shuffle(col, side), row, rows), left), 0)
    shape = (6 * spare, side)
    row, col = iota(shape, 0) // spare, iota(shape, 1)
    sr_ref[p] = cosines(shuffle(col, side), layer_place(row, rows), rows)
    shape = (6 * spare, 2 * side)
    row, col = iota(shape, 0) // spare, iota(shape, 1)
    sc_ref[p] = cosines(col % side, layer_place(row, cols), cols)


def tables_kernel(boxes, faces, here, spot, w_ref, c_ref, ws_ref, cs_ref):
    side = w_ref.shape[1]

    def body(p, carry):
        rows, cols = boxes[0, p], boxes[1, p]
        shape = (side, side)
        row, col = iota(shape, 0), shuffle(iota(shape, 1), side)
        high, low = split(cosines(col, shuffle(row, side), rows))
        w_ref[p] = jnp.concatenate([high, high, low], 1)
        high, low = split(cosines(col, row, rows))
        ws_ref[p, :side] = jnp.concatenate([high, high, low], 1)
        shape = (16, side)
        row, col = iota(shape, 0), shuffle(iota(shape, 1), side)
        high, low = split(cosines(col, layer_place(row, rows), rows))
        ws_ref[p, side:] = jnp.concatenate([high, high, low], 1)
        shape = (side, 2 * side)
        row, wide = iota(shape, 0), iota(shape, 1)
        left, col = wide < side, wide % side
        straight = jnp.concatenate(paired(cosines(row, col, cols), left), 0)
        c_ref[p] = straight
        cs_ref[p, :, : 2 * side] = straight
        values = cosines(row, layer_place(wide % 8, cols), cols)
        values = jnp.where((wide < 16) & (wide % 8 < 6), values, 0.0)
        cs_ref[p, :, 2 * side :] = jnp.concatenate(paired(values, wide < 8), 0)
        return carry

    lax.fori_loop(0, w_ref.shape[0], body, 0)


def make_tables(boxes, faces, here, spot, side):
    holders = boxes.shape[1]
    shapes = [
        ((holders, side, 3 * side), jnp.bfloat16),
        ((holders, 6 * side, 2 * side), jnp.bfloat16),
        ((holders, side + 16, 3 * side), jnp.bfloat16),
        ((holders, 6 * side, 4 * side), jnp.bfloat16),
    ]
    return pl.pallas_call(
        tables_kernel,
        grid_spec=pltpu.PrefetchScalarGridSpec(
            num_scalar_prefetch=4,
            grid=(1,),
            in_specs=[],
            out_specs=[whole(shape) for shape, _ in shapes],
        ),
        out_shape=[jax.ShapeDtypeStruct(*shape) for shape in shapes],
        name="tables",
        compiler_params=ROOM,
        cost_estimate=pl.CostEstimate(flops=10**9, bytes_accessed=5 * 10**6, transcendentals=0),
    )(boxes, faces, here, spot)


def mix_kernel(total, spot, own_ref, other_ref, *refs):
    *out_refs, t_ref = refs
    planes, holders, _ = own_ref.shape
    early = out_refs[0].shape[0]
    shares = total // planes
    count = planes * holders
    me = spot[0]
    masks = near_masks(shares)

    @pl.when(pl.program_id(0) == 0)
    def _():
        for k, mask in enumerate(masks):
            for odd in range(2):
                shape = (count, count)
                row, col = iota(shape, 0), iota(shape, 1)
                slot = col // holders
                half = planes // 2
                where_from = jnp.where(slot < half, me * planes, (me ^ 1) * planes - planes)
                mode = where_from + 2 * slot + odd
                place = (me ^ mask) * planes + row // holders
                values = cosines(mode, place, total)
                values = jnp.where(row % holders == col % holders, values, 0.0)
                t_ref[odd, k * count : (k + 1) * count] = thrice(values)

    mixed = []
    for odd in range(2):
        picked = [r[z] for r in (own_ref, other_ref) for z in range(odd, planes, 2)]
        high, low = split(jnp.concatenate(picked, 0))
        mixed.append(dot(t_ref[odd], jnp.concatenate([high, high, low], 0)))
    for k in range(len(masks)):
        near, far = out_refs[4 * k : 4 * k + 2], out_refs[4 * k + 2 : 4 * k + 4]
        for z in range(planes):
            at = slice((k * planes + z) * holders, (k * planes + z + 1) * holders)
            even, odd = mixed[0][at], mixed[1][at]
            for refs, n, value in ((near, z, even + odd), (far, planes - 1 - z, even - odd)):
                refs[n // early][n % early] = value


def near_masks(shares):
    top = shares // 2
    return [m for m in range(top) if m & 1 == 0]


def mix(spot, own, other, shares, front):
    planes, holders, cells = own.shape
    cells = cells - front
    count = len(near_masks(shares))
    step = math.gcd(front, cells)
    sizes = [planes - GROUP, GROUP] * (2 * count)
    block = lambda i, s: (0, 0, i)
    later = lambda i, s: (0, 0, i + front // step)
    outs = pl.pallas_call(
        functools.partial(mix_kernel, shares * planes),
        grid_spec=pltpu.PrefetchScalarGridSpec(
            num_scalar_prefetch=1,
            grid=(cells // step,),
            in_specs=[pl.BlockSpec((planes, holders, step), later)] * 2,
            out_specs=[pl.BlockSpec((size, holders, step), block) for size in sizes],
            scratch_shapes=[
                pltpu.VMEM((2, count * planes * holders, 3 * planes * holders), jnp.bfloat16)
            ],
        ),
        out_shape=[jax.ShapeDtypeStruct((size, holders, cells), jnp.float32) for size in sizes],
        name="mix",
        compiler_params=ROOM,
        cost_estimate=pl.CostEstimate(
            flops=3 * 10**9, bytes_accessed=16 * planes * holders * cells, transcendentals=0
        ),
    )(spot, own, other)
    return [list(outs[2 * k : 2 * k + 2]) for k in range(2 * count)]


def exchange_kernel(total, places, boxes, out_ref, now_ref, prev_ref, *refs):
    field_refs = refs[: len(places)]
    r_ref, first_ref, kept_ref, gain_ref, *table_refs = refs[len(places) :]
    *table_refs, land_ref, t_ref, send_sem, recv_sem = table_refs
    doms = out_ref.shape[0]
    planes, holders, cells = now_ref.shape
    front = first_ref.shape[2]
    here = lax.axis_index("dom")
    me = lax.axis_index("height")
    count = planes * holders

    barrier = pltpu.get_barrier_semaphore()
    for m in range(1, doms):
        goal = {"dom": lax.rem(here + m, doms)}
        pl.semaphore_signal(barrier, inc=1, device_id=goal, device_id_type=pl.DeviceIdType.MESH)
    for k, mask in enumerate(places):
        shape = (count, count)
        row, col = iota(shape, 0), iota(shape, 1)
        values = cosines((me ^ mask) * planes + col // holders, me * planes + row // holders, total)
        high, low = split(jnp.where(row % holders == col % holders, values, 0.0))
        for n, part in enumerate((high, low, high)):
            at = n * len(places) + k
            t_ref[:, at * count : (at + 1) * count] = part
    pl.semaphore_wait(barrier, doms - 1)
    copies = []
    for m in range(1, doms):
        copy = pltpu.make_async_remote_copy(
            src_ref=out_ref.at[m],
            dst_ref=land_ref.at[m],
            send_sem=send_sem.at[m],
            recv_sem=recv_sem.at[m],
            device_id={"dom": lax.rem(here + m, doms)},
            device_id_type=pl.DeviceIdType.MESH,
        )
        copy.start()
        copies.append(copy)
    r_ref[0] = out_ref[0]

    step = front // 4
    for n in range(4):
        at = slice(n * step, (n + 1) * step)
        x = jnp.concatenate([ref[:, :, at].reshape(count, step) for ref in field_refs], 0)
        high, low = split(x)
        mixed = dot(t_ref[...], jnp.concatenate([high, high, low], 0))
        first_ref[:, :, at] = mixed.reshape(planes, holders, step)

    scale = (math.pi * TIME_STEP / 2) ** 2
    side = math.isqrt(cells)
    cell = iota((holders, cells), 1)
    wave_row, wave_col = cell // side, cell % side
    holder = iota((holders, 1), 0)
    extent_row = jnp.zeros((holders, 1), jnp.int32)
    extent_col = jnp.zeros((holders, 1), jnp.int32)
    for p in range(holders):
        extent_row = jnp.where(holder == p, boxes[0, p], extent_row)
        extent_col = jnp.where(holder == p, boxes[1, p], extent_col)
    ratio_row = wave_row.astype(jnp.float32) / extent_row.astype(jnp.float32)
    ratio_col = wave_col.astype(jnp.float32) / extent_col.astype(jnp.float32)
    inside = (wave_row < extent_row) & (wave_col < extent_col)
    base = scale * (ratio_row * ratio_row + ratio_col * ratio_col)
    gain_ref[0] = jnp.where(inside, base, -1.0)
    kept_ref[0] = jnp.where(inside, base, -1.0)

    def pace(n, carry):
        z = planes - 1 - n
        base = gain_ref[0]
        depth = (me * planes + z).astype(jnp.float32) / total
        quarter = base + scale * (depth * depth)
        ratio = jnp.float32(SERIES[-1])
        for coefficient in SERIES[-2::-1]:
            ratio = ratio * quarter + coefficient
        ratio = ratio * ratio
        kept = (2.0 - 4.0 * quarter * ratio) * now_ref[z] - prev_ref[z]
        kept_ref[z] = jnp.where(base >= 0.0, kept, 0.0)
        gain_ref[z] = jnp.where(base >= 0.0, (TIME_STEP * TIME_STEP) * ratio, 0.0)
        return carry

    lax.fori_loop(0, planes, pace, 0)

    def table(p, carry):
        force_tables(p, boxes, *table_refs)
        return carry

    lax.fori_loop(0, holders, table, 0)
    for copy in copies:
        copy.wait_recv()
    for m in range(1, doms):
        r_ref[m] = land_ref[m]
    for copy in copies:
        copy.wait_send()


def exchange(boxes, outgoing, now, prev, fields, places, front, shares):
    planes, holders, _ = now.shape
    count = planes * holders
    doms = outgoing.shape[0]
    field = pl.BlockSpec((planes, holders, front), lambda i: (0, 0, 0))
    side, spare = outgoing.shape[3] // 2, outgoing.shape[2]
    outs = [outgoing.shape, (planes, holders, front), now.shape, now.shape]
    outs = [(shape, jnp.float32) for shape in outs]
    outs += [((holders, 6 * side, 2 * side), jnp.bfloat16)] * 2
    outs += [((holders, 6 * spare, n * side), jnp.float32) for n in (1, 2)]
    return pl.pallas_call(
        functools.partial(exchange_kernel, shares * planes, places),
        grid=(1,),
        in_specs=[pl.BlockSpec(memory_space=pltpu.SMEM)]
        + [whole(o.shape) for o in (outgoing, now, prev)]
        + [field] * len(fields),
        out_specs=[whole(shape) for shape, _ in outs],
        out_shape=[jax.ShapeDtypeStruct(*out) for out in outs],
        scratch_shapes=[
            pltpu.VMEM(outgoing.shape, jnp.float32),
            pltpu.VMEM((count, 3 * len(places) * count), jnp.bfloat16),
            pltpu.SemaphoreType.DMA((doms,)),
            pltpu.SemaphoreType.DMA((doms,)),
        ],
        name="exchange",
        compiler_params=pltpu.CompilerParams(
            vmem_limit_bytes=24 * 2**20, collective_id=0, has_side_effects=True
        ),
        cost_estimate=pl.CostEstimate(
            flops=10**10, bytes_accessed=20 * planes * holders * front, transcendentals=0
        ),
    )(boxes, outgoing, now, prev, *fields)


def columns_of(planes, p, low, side):
    cols = []
    for k in range(len(planes) // 2):
        one, two = planes[2 * k][p], planes[2 * k + 1][p]
        top = jnp.where(low, one, pltpu.roll(two, side, 1))
        bottom = jnp.where(low, pltpu.roll(one, side, 1), two)
        cols.append(jnp.concatenate([top, bottom], 0))
    high, rest = split(jnp.concatenate(cols, 1))
    return jnp.concatenate([high, rest, high], 0)


def unpaired(top, bottom, low, side):
    one = jnp.where(low, top, pltpu.roll(bottom, side, 1))
    two = jnp.where(low, pltpu.roll(top, side, 1), bottom)
    return one, two


def sides_kernel(x_ref, w_ref, c_ref, s_ref):
    group, holders, cells = x_ref.shape
    side = math.isqrt(cells)
    half = side // 2
    wide = 2 * side
    low = iota((half, wide), 1) < side
    first = iota((side, wide), 1) < 8
    planes = [x_ref[z].reshape(holders, half, wide) for z in range(group)]
    pairs = group // 2
    base = pl.program_id(0) * pairs
    rows = side + 16
    for p in range(holders):
        v = dot(w_ref[p], columns_of(planes, p, low, side))
        v = jnp.concatenate([v[:, wide * k : wide * (k + 1)] for k in range(pairs)], 0)
        q = dot(thrice(v), c_ref[p])
        ends = [q[rows * k : rows * k + side, wide:] for k in range(pairs)]
        upper = jnp.where(first, ends[0], pltpu.roll(ends[1], 8, 1))
        lower = jnp.where(first, pltpu.roll(ends[0], wide - 8, 1), ends[1])
        turned = jnp.transpose(jnp.concatenate([upper, lower], 0))
        for k in range(pairs):
            for s in range(6):
                at = rows * k + side + s
                s_ref[p, s, pl.ds(base + k, 1), :] = q[at : at + 1, :wide]
                s_ref[p, 6 + s, pl.ds(base + k, 1), :] = turned[8 * k + s : 8 * k + s + 1]


def find_sides(modes, weights, columns, spare):
    planes, holders, cells = modes.shape
    wide = 2 * math.isqrt(cells)
    shape = (holders, SIDES, spare, wide)
    return pl.pallas_call(
        sides_kernel,
        grid=(planes // GROUP,),
        in_specs=[
            pl.BlockSpec((GROUP, holders, cells), lambda i: (i, 0, 0)),
            whole(weights.shape),
            whole(columns.shape),
        ],
        out_specs=whole(shape),
        out_shape=jax.ShapeDtypeStruct(shape, jnp.float32),
        name="sides",
        compiler_params=ROOM,
        cost_estimate=pl.CostEstimate(
            flops=6 * 10**9, bytes_accessed=4 * planes * holders * cells, transcendentals=0
        ),
    )(modes, weights, columns)


def faces_kernel(table, place_ref, s_ref, o_ref, count):
    doms, tiles, spare, wide = o_ref.shape
    slots = (tiles - 1) // 3
    place = iota((spare, wide), 1) % (wide // 2)
    lane = iota((1, wide), 1)
    o_ref[...] = jnp.zeros_like(o_ref)
    for d in range(doms):
        count[d] = 0

    def body(r, carry):
        length = table[3, r]
        part = jnp.minimum(table[0, r], s_ref.shape[0] - 1)
        facing = jnp.minimum(table[1, r], 3)
        to = jnp.minimum(table[4, r], doms - 1) - place_ref[0]
        to = jnp.where(to < 0, to + doms, to)
        seen = count[to]
        count[to] = seen + jnp.minimum(length, 1)
        slot = jnp.minimum(seen, slots - 1)
        for j in range(3):
            moved = pltpu.roll(s_ref[part, facing * 3 + j], wide - table[2, r], 1)
            o_ref[to, slot * 3 + j] += jnp.where(place < length, moved, 0.0)
        label = jnp.where(lane == 0, table[5, r], jnp.where(lane == 1, table[6, r], table[7, r]))
        label = jnp.where(lane == 3, length, label) * jnp.minimum(length, 1)
        o_ref[to, tiles - 1, pl.ds(slot, 1), :] += label.astype(jnp.float32)
        return carry

    lax.fori_loop(0, table.shape[1], body, 0, unroll=4)


def find_faces(sides, table, here, doms):
    _, _, spare, wide = sides.shape
    slots = max(2, table.shape[1] // doms)
    shape = (doms, 3 * slots + 1, spare, wide)
    return pl.pallas_call(
        faces_kernel,
        grid_spec=pltpu.PrefetchScalarGridSpec(
            num_scalar_prefetch=2,
            grid=(1,),
            in_specs=[whole(sides.shape)],
            out_specs=whole(shape),
            scratch_shapes=[pltpu.SMEM((doms,), jnp.int32)],
        ),
        out_shape=jax.ShapeDtypeStruct(shape, jnp.float32),
        name="faces",
        compiler_params=ROOM,
        cost_estimate=pl.CostEstimate(flops=10**8, bytes_accessed=10**6, transcendentals=0),
    )(table, here, sides)


def force_kernel(
    pairs, labels, r_ref, s_ref, ct_ref, rt_ref, sr_ref, sc_ref, kept_ref, gain_ref, o_ref, f_ref,
    m_ref,
):
    group, holders, cells = kept_ref.shape
    doms, tiles, spare, wide = r_ref.shape
    side = wide // 2
    half = side // 2
    slots = (tiles - 1) // 3

    @pl.when(pl.program_id(0) == 0)
    def _():
        f_ref[...] = jnp.zeros_like(f_ref)
        place = iota((spare, wide), 1) % side

        for d in range(doms):
            for n in range(slots):
                at = d * slots + n
                part, facing, start = labels[at, 0], labels[at, 1], labels[at, 2]
                mask = (place >= start) & (place < start + labels[at, 3])
                jumps = []
                for j in range(3):
                    moved = pltpu.roll(r_ref[d, n * 3 + j], start, 1)
                    jumps.append(jnp.where(mask, moved - s_ref[part, facing * 3 + j], 0.0))
                for i in range(3):
                    push = sum(STENCIL[i + j] * jumps[j] for j in range(3 - i))
                    f_ref[part, facing * 3 + i] += push
        shape = (6 * spare, wide)
        pair = iota(shape, 0) % spare
        left = iota(shape, 1) < side

        def spread(p, carry):
            f = f_ref[p, :6].reshape(6 * spare, wide)
            g = f_ref[p, 6:].reshape(6 * spare, wide)
            fc = dot(thrice(f), ct_ref[p])
            gr = dot(thrice(g), rt_ref[p])
            near = jnp.concatenate([sr_ref[p], gr[:, :side], gr[:, side:]], 0)
            sc = sc_ref[p]
            sc_left = jnp.where(left, sc, 0.0)
            sc_right = jnp.where(left, 0.0, sc)
            highs, lows = zip(*(split(t) for t in (fc, sc_left, sc_right)))
            masks = [jnp.where(pair == k, 1.0, 0.0).astype(jnp.bfloat16) for k in range(pairs)]
            far_high, far_low = (
                jnp.concatenate(
                    [jnp.concatenate([t * mask for t in parts], 0) for mask in masks], 1
                )
                for parts in (highs, lows)
            )
            near_high, near_low = split(near)
            out = lax.dot_general(
                jnp.concatenate([near_high, near_low, near_high], 0),
                jnp.concatenate([far_high, far_high, far_low], 0),
                (((0,), (0,)), ((), ())),
                preferred_element_type=jnp.float32,
            )
            for k in range(pairs):
                m_ref[k, p] = out[:, k * wide : (k + 1) * wide]
            return carry

        lax.fori_loop(0, holders, spread, 0)

    low = iota((half, wide), 1) < side
    for k in range(group // 2):
        at = pl.program_id(0) * (group // 2) + k
        outs = [
            unpaired(m_ref[at, p, :half], m_ref[at, p, half:], low, side) for p in range(holders)
        ]
        for c in range(2):
            z = 2 * k + c
            force = jnp.stack([out[c] for out in outs], 0).reshape(holders, cells)
            o_ref[z] = kept_ref[z] + gain_ref[z] * force


def advance(received, sides, tables, kept, gain):
    planes, holders, cells = kept.shape
    doms, tiles, spare, wide = received.shape
    slots = (tiles - 1) // 3
    labels = received[:, tiles - 1, :slots, :4].astype(jnp.int32).reshape(doms * slots, 4)
    pairs = planes // 2
    operands = (received, sides, *tables)
    block = pl.BlockSpec((GROUP, holders, cells), lambda i, *_: (i, 0, 0))
    return pl.pallas_call(
        functools.partial(force_kernel, pairs),
        grid_spec=pltpu.PrefetchScalarGridSpec(
            num_scalar_prefetch=1,
            grid=(planes // GROUP,),
            in_specs=[whole(o.shape) for o in operands] + [block, block],
            out_specs=block,
            scratch_shapes=[
                pltpu.VMEM((holders, SIDES, spare, wide), jnp.float32),
                pltpu.VMEM((pairs, holders, wide // 2, wide), jnp.float32),
            ],
        ),
        out_shape=jax.ShapeDtypeStruct(kept.shape, jnp.float32),
        name="force",
        compiler_params=ROOM,
        cost_estimate=pl.CostEstimate(
            flops=8 * 10**9, bytes_accessed=12 * planes * holders * cells, transcendentals=0
        ),
    )(labels, *operands, kept, gain)


def cells_kernel(w_ref, c_ref, *refs):
    *part_refs, q_ref = [ref for ref in refs if ref is not None]
    group, holders, cells = q_ref.shape
    side = math.isqrt(cells)
    half = side // 2
    wide = 2 * side
    low = iota((half, wide), 1) < side
    first_ref, *part_refs = part_refs
    planes = []
    for z in range(group):
        rest = sum(ref[z] for ref in part_refs)
        planes.append(jnp.concatenate([first_ref[z], rest], 1).reshape(holders, half, wide))
    outs = [[] for _ in range(group)]
    for p in range(holders):
        v = dot(w_ref[p], columns_of(planes, p, low, side))
        v = jnp.concatenate([v[:, wide * k : wide * (k + 1)] for k in range(group // 2)], 0)
        q = dot(thrice(v), c_ref[p])
        for k in range(group // 2):
            pair = q[side * k : side * (k + 1)]
            outs[2 * k], outs[2 * k + 1] = (
                out + [new]
                for out, new in zip(outs[2 * k : 2 * k + 2], unpaired(pair[:half], pair[half:], low, side))
            )
    for z in range(group):
        q_ref[z] = jnp.stack(outs[z], 0).reshape(holders, cells)


def resumed_kernel(buffer_ref, *refs):
    cells_kernel(*refs)


def to_cells(first, parts, weights, columns, chunk, buffer):
    planes, holders, front = first.shape
    size, _, rest = parts[0].shape
    cells = rest + front
    operands = [weights, columns, first, *parts]
    specs = [whole(weights.shape), whole(columns.shape)]
    specs.append(pl.BlockSpec((GROUP, holders, front), lambda i: (i + chunk, 0, 0)))
    specs += [pl.BlockSpec((GROUP, holders, rest), lambda i: (i, 0, 0))] * len(parts)
    kernel, aliases = cells_kernel, {}
    if buffer is not None:
        operands = [buffer] + operands
        specs = [pl.BlockSpec(memory_space=pl.ANY)] + specs
        kernel, aliases = resumed_kernel, {0: 0}
    return pl.pallas_call(
        kernel,
        grid=(size // GROUP,),
        in_specs=specs,
        out_specs=pl.BlockSpec((GROUP, holders, cells), lambda i: (i + chunk, 0, 0)),
        out_shape=jax.ShapeDtypeStruct((planes, holders, cells), jnp.float32),
        input_output_aliases=aliases,
        name="cells",
        compiler_params=ROOM,
        cost_estimate=pl.CostEstimate(
            flops=10**8 * size * 5, bytes_accessed=12 * size * holders * cells, transcendentals=0
        ),
    )(*operands)


def on_device(modes_now, modes_prev, partition_boxes, face_table):
    planes, _, cells = modes_now.shape
    side = math.isqrt(cells)
    shares = lax.axis_size("height")
    doms = lax.axis_size("dom")
    spare = -(-planes // 16) * 8
    spot = lax.axis_index("height").astype(jnp.int32).reshape(1)
    here = lax.axis_index("dom").astype(jnp.int32).reshape(1)
    boxes, listed = partition_boxes.T, face_table.T
    swap = lambda size, mask: [(h, h ^ mask) for h in range(size)]
    front = cells // 4
    raw, whole_modes = lax.optimization_barrier((modes_now[:, :, :front], modes_now))
    far = list(range(2, shares, 2))
    arrived = [lax.ppermute(raw, "height", swap(shares, mask)) for mask in far]
    other = lax.ppermute(whole_modes, "height", swap(shares, 1))
    w, c, ws, cs = make_tables(boxes, listed, here, spot, side)
    parts = mix(spot, modes_now, other, shares, front)
    kept, sent = parts[0], [[], []]
    for k in range(2):
        for m, part in enumerate(parts[1:], 1):
            goal = near_masks(shares)[m // 2] ^ (shares - 1) * (m % 2)
            sent[k].append(lax.ppermute(part[k], "height", swap(shares, goal)))
    sides = find_sides(modes_now, ws, cs, spare)
    *arrived, sides = lax.optimization_barrier((*arrived, sides))
    passed = [lax.ppermute(x, "height", swap(shares, 1)) for x in arrived]
    outgoing = find_faces(sides, listed, here, doms)
    fields = [modes_now, other, *arrived, *passed]
    places = [0, 1, *far, *(mask ^ 1 for mask in far)]
    received, first, steady, gain, *tables = exchange(
        boxes, outgoing, modes_now, modes_prev, fields, places, front, shares
    )
    new_modes = advance(received, sides, tables, steady, gain)
    pressure = None
    kept[0], new_modes = lax.optimization_barrier((kept[0], new_modes))
    for k in range(2):
        chunk = k * (planes // GROUP - 1)
        pressure = to_cells(first, [kept[k]] + sent[k], w, c, chunk, pressure)
    return (new_modes, pressure)


def solution(mesh):
    placed = (P("height", "dom", None), P("height", "dom", None), P("dom", None), P("dom", None))

    return jax.shard_map(
        on_device,
        mesh=mesh,
        in_specs=placed,
        out_specs=(P("height", "dom", None), P("height", "dom", None)),
        check_vma=False,
    )
```
